128 devices in a mesh: head: 4 (over y_hi, core), seq: 32 (over x, z, y_lo).
Axes of the slice: x: 4, y: 4 (y_hi: 2, y_lo: 2; y = y_hi * 2 + y_lo), z: 4, core: 2. Of those that a mesh axis runs over, the one named last changes fastest.
Arguments:
- queries: bfloat16 [32768, 4096], P('seq', 'head'), may hold values from -6 to 6
- keys: bfloat16 [32768, 512], P('seq', 'head'), may hold values from -6 to 6
- values: bfloat16 [32768, 512], P('seq', 'head'), may hold values from -6 to 6
- vertical: int32 [32, 8], P('head'), may hold values from 0 to 255, as said below
- slash: int32 [32, 8], P('head'), may hold values from 1 to 28, as said below
Outputs:
- attended: bfloat16 [32768, 4096], P(('seq', 'head'))
The draws below stay inside these ranges and needn't reach their ends.
Inputs may be any that keep to these rules, and one draw needn't show every extreme that they name: `vertical`: each row names 8 different blocks. Within each group of 8 consecutive rows, the different blocks named that lie in one slab (blocks s * 8 to s * 8 + 7) number at most 4, and exactly 4 in some slab. `slash`: each row names 8 different offsets.
All inputs are finite; a program needn't handle non-finite values.
Results may differ from the reference program's by a relative error of at most 0.0033.
Values may be sent and summed in bfloat16 or wider, within the bound.
A program may use at most 128 MiB of HBM per device.

```python
import math
import jax
import jax.numpy as jnp
from jax import lax

HD = 128
QUERY_PER_GROUP = 8
BLK = 128
VERTICAL_BLOCKS = 8
SLASH_OFFSETS = 8
LARGEST_OFFSET = 28
CAP = 4
GROUPS = 4
HEADS = 32
BLK_DEV = 8
SLABS = 32
SEQ = 32768
BLOCKS = 256


def draw_queries(key, part):
    own_key = jax.random.fold_in(key, 11)
    drawn = jnp.clip(1.5 * jax.random.normal(own_key, (SEQ, GROUPS, QUERY_PER_GROUP, HD), jnp.float32), -6.0, 6.0)
    return drawn.reshape(SEQ, HEADS * HD).astype(jnp.bfloat16)


def draw_keys(key, part):
    own_key = jax.random.fold_in(key, 12)
    drawn = jnp.clip(1.5 * jax.random.normal(own_key, (SEQ, GROUPS, HD), jnp.float32), -6.0, 6.0)
    return drawn.reshape(SEQ, GROUPS * HD).astype(jnp.bfloat16)


def vertical_group(key):
    key_count, key_full, key_order, key_pick = jax.random.split(key, 4)
    slab_ids = jnp.arange(SLABS, dtype=jnp.int32)
    counts = jax.random.randint(key_count, (SLABS,), 1, CAP + 1)
    fullest = jax.random.randint(key_full, (), 0, SLABS)
    counts = jnp.where(slab_ids == fullest, CAP, counts)
    order_scores = jax.random.randint(key_order, (SLABS, BLK_DEV), 0, 4096) * BLK_DEV + jnp.arange(BLK_DEV, dtype=jnp.int32)[None, :]
    ranks = jnp.argsort(jnp.argsort(order_scores, axis=1), axis=1)
    inside = ranks < counts[:, None]
    mandatory_blocks = (inside & (slab_ids[:, None] == fullest)).reshape(BLOCKS)
    inside = inside.reshape(BLOCKS)
    selected_indices = jax.random.randint(key_pick, (QUERY_PER_GROUP, BLOCKS), 0, 65536) * BLOCKS + jnp.arange(BLOCKS, dtype=jnp.int32)[None, :] + 1
    selected_indices = jnp.where(inside[None, :], selected_indices, 0)
    extra_score = jnp.where((jnp.arange(QUERY_PER_GROUP)[:, None] == 0) & mandatory_blocks[None, :], 1 << 29, 0)
    leftover_slots, selected_blocks = lax.top_k(selected_indices + extra_score, VERTICAL_BLOCKS)
    return selected_blocks.astype(jnp.int32)


def draw_vertical(key, part):
    group_keys = jax.random.split(jax.random.fold_in(key, 31), GROUPS)
    return jax.vmap(vertical_group)(group_keys).reshape(HEADS, VERTICAL_BLOCKS).astype(jnp.int32)


def draw_slash(key, part):
    block_scores = jax.random.randint(jax.random.fold_in(key, 41), (HEADS, LARGEST_OFFSET), 0, 65536) * LARGEST_OFFSET + jnp.arange(LARGEST_OFFSET, dtype=jnp.int32)[None, :] + 1
    per_head_rows = jnp.arange(HEADS)[:, None]
    offset_columns = jnp.arange(LARGEST_OFFSET)[None, :]
    extra_score = jnp.where((per_head_rows == 0) & (offset_columns == LARGEST_OFFSET - 1), 1 << 28, 0)
    extra_score = extra_score + jnp.where((per_head_rows == 1) & (offset_columns == 0), 1 << 28, 0)
    leftover_slots, selected_blocks = lax.top_k(block_scores + extra_score, SLASH_OFFSETS)
    return (selected_blocks + 1).astype(jnp.int32)


def block_levels(key, extent, pieces, least, largest):
    factor_of, own = 1.0, jax.random.fold_in(key, 6)
    for position, shards_of in pieces:
        steps = jnp.exp(jax.random.uniform(jax.random.fold_in(own, position), (shards_of,), jnp.float32, least / len(pieces), largest / len(pieces)))
        factor_of = factor_of * jnp.repeat(steps, extent[position] // shards_of).reshape([-1 if axis == position else 1 for axis in range(len(extent))])
    return factor_of


def normal_values(rng, dims, scale, limit, cuts=(), held_as=jnp.bfloat16):
    level = block_levels(rng, dims, cuts, -0.22, 0.18) if cuts else 1.0
    values = jax.random.normal(rng, dims, jnp.float32) * scale * level
    return jnp.minimum(jnp.maximum(values, -limit), limit).astype(held_as)


def setup_inputs(seed: int = 0) -> dict:
    key_list = jax.random.split(jax.random.key(seed), 6)
    return {
        "queries": draw_queries(jax.random.fold_in(key_list[5], 71), 0),
        "keys": draw_keys(jax.random.fold_in(key_list[5], 71), 0),
        "values": normal_values(key_list[2], (SEQ, GROUPS * HD), 1.0, 6.0, ((0, 32), (1, 4))),
        "vertical": draw_vertical(jax.random.fold_in(key_list[5], 71), 0),
        "slash": draw_slash(jax.random.fold_in(key_list[5], 71), 0),
    }


NEG = -1e+30

def attend(query_block, diag_kv, slash_kv, column_kv, slash_ok, column_ok):
    block_count, block_width, head_width = query_block.shape
    slash_count = slash_kv.shape[1]
    column_count = column_kv.shape[0]
    score_scale = 1.0 / math.sqrt(head_width)
    causal = jnp.arange(block_width)[:, None] >= jnp.arange(block_width)[None, :]
    diag_scores = jnp.einsum('ird,icd->irc', query_block, diag_kv[..., :head_width]) * score_scale
    diag_scores = jnp.where(causal[None], diag_scores, NEG)
    slash_scores = jnp.einsum('ird,ijcd->irjc', query_block, slash_kv[..., :head_width]) * score_scale
    slash_scores = jnp.where(slash_ok[:, None, :, None], slash_scores, NEG).reshape(block_count, block_width, slash_count * block_width)
    column_scores = jnp.einsum('ird,jcd->irjc', query_block, column_kv[..., :head_width]) * score_scale
    column_scores = jnp.where(column_ok[:, None, :, None], column_scores, NEG).reshape(block_count, block_width, column_count * block_width)
    block_scores = jnp.concatenate([diag_scores, slash_scores, column_scores], axis=2)
    row_top = lax.optimization_barrier(jnp.max(block_scores, axis=2, keepdims=True))
    weights = jnp.exp(block_scores - row_top)
    row_total = lax.optimization_barrier(jnp.sum(weights, axis=2))
    rounded = lax.optimization_barrier(weights.astype(jnp.bfloat16)).astype(jnp.float32)
    split_one = block_width
    split_two = block_width + slash_count * block_width
    w_diag = rounded[:, :, :split_one]
    w_slash = rounded[:, :, split_one:split_two].reshape(block_count, block_width, slash_count, block_width)
    w_column = rounded[:, :, split_two:].reshape(block_count, block_width, column_count, block_width)
    mixed_sum = jnp.einsum('irc,icd->ird', w_diag, diag_kv[..., head_width:])
    mixed_sum = mixed_sum + jnp.einsum('irjc,ijcd->ird', w_slash, slash_kv[..., head_width:])
    mixed_sum = mixed_sum + jnp.einsum('irjc,jcd->ird', w_column, column_kv[..., head_width:])
    return (mixed_sum / row_total[:, :, None]).astype(jnp.bfloat16)

def reference(queries, keys, values, vertical, slash):
    seq_rows = queries.shape[0]
    block_total = seq_rows // BLK
    joined = jnp.concatenate([keys.reshape(seq_rows, GROUPS, HD), values.reshape(seq_rows, GROUPS, HD)], axis=2)
    block_ids = jnp.arange(block_total, dtype=jnp.int32)

    def one_head(head_index):
        group_index = head_index // QUERY_PER_GROUP
        query_block = lax.dynamic_slice_in_dim(queries, head_index * HD, HD, 1).astype(jnp.float32).reshape(block_total, BLK, HD)
        group_kv = lax.dynamic_index_in_dim(joined, group_index, 1, keepdims=False).astype(jnp.float32).reshape(block_total, BLK, 2 * HD)
        padded = jnp.concatenate([jnp.zeros((LARGEST_OFFSET, BLK, 2 * HD), jnp.float32), group_kv], axis=0)
        offsets = lax.dynamic_index_in_dim(slash, head_index, 0, keepdims=False)
        columns = lax.dynamic_index_in_dim(vertical, head_index, 0, keepdims=False)
        slash_index = (LARGEST_OFFSET + block_ids[:, None] - offsets[None, :]).astype(jnp.int32)
        slash_kv = jnp.take(padded, slash_index, axis=0)
        slash_ok = block_ids[:, None] - offsets[None, :] >= 0
        column_kv = jnp.take(group_kv, columns.astype(jnp.int32), axis=0)
        covered = jnp.any(block_ids[:, None, None] - columns[None, :, None] == offsets[None, None, :], axis=2)
        column_ok = (columns[None, :] < block_ids[:, None]) & jnp.logical_not(covered)
        return attend(query_block, group_kv, slash_kv, column_kv, slash_ok, column_ok)
    outputs = lax.map(one_head, jnp.arange(HEADS, dtype=jnp.int32))
    return jnp.transpose(outputs, (1, 2, 0, 3)).reshape(seq_rows, HEADS * HD)
```

```python
import functools, math
import jax, jax.numpy as jnp
from jax import lax
from jax.experimental import pallas as pl
from jax.experimental.pallas import tpu as pltpu
from jax.sharding import Mesh
from jax.sharding import PartitionSpec as P

BLK = 128
NEG = -1e30
BACK = 28
F32 = jnp.float32
BF16 = jnp.bfloat16
SCALE2 = math.log2(math.e) / math.sqrt(128.0)


def dot(a, b):
    return jnp.dot(a, b, preferred_element_type=F32)


def lane_max(parts):
    top = parts[0]
    for part in parts[1:]:
        top = jnp.maximum(top, part)
    return jnp.max(top, axis=1, keepdims=True)


def lane_sum(parts):
    total = parts[0]
    for part in parts[1:]:
        total = total + part
    return jnp.sum(total, axis=1, keepdims=True)


def near_step(h, i, slab, slash_ref, q_ref, ext_ref, acc_ref, top_ref, sum_ref):
    rows = pl.ds(pl.multiple_of(i * BLK, BLK), BLK)
    q = q_ref[h, rows, :]
    row = lax.broadcasted_iota(jnp.int32, (BLK, BLK), 0)
    col = lax.broadcasted_iota(jnp.int32, (BLK, BLK), 1)
    own = BACK + i
    scores = [jnp.where(row >= col, dot(q, ext_ref[own, 0]), NEG)]
    blocks = [own]
    for n in range(0, 8, 2):
        pair, bias = [], []
        for k in (n, n + 1):
            off = slash_ref[h, k]
            ok = slab * 8 + i - off >= 0
            pair.append(jnp.where(ok, own - off, own))
            bias.append(jnp.where(ok, 0.0, NEG).astype(F32))
        both = dot(q, jnp.concatenate([ext_ref[pair[0], 0], ext_ref[pair[1], 0]], axis=1))
        scores.append(both[:, :BLK] + bias[0])
        scores.append(both[:, BLK:] + bias[1])
        blocks += pair
    top = lane_max(scores)
    weights = [jnp.exp2((s - top) * SCALE2) for s in scores]
    acc = dot(weights[0].astype(BF16), ext_ref[blocks[0], 1])
    for n in range(1, 9, 2):
        p = jnp.concatenate([weights[n].astype(BF16), weights[n + 1].astype(BF16)], axis=1)
        v = jnp.concatenate([ext_ref[blocks[n], 1], ext_ref[blocks[n + 1], 1]], axis=0)
        acc = acc + dot(p, v)
    acc_ref[h, rows, :] = acc
    top_ref[h, rows, :] = top
    sum_ref[h, rows, :] = lane_sum(weights)


def far_step(h, i, slab, slash_ref, vert_ref, pos_ref, q_ref, far_ref, acc_ref, top_ref, sum_ref, out_ref):
    rows = pl.ds(pl.multiple_of(i * BLK, BLK), BLK)
    q = q_ref[h, rows, :]
    mine = slab * 8 + i
    bias, places = [], []
    for k in range(8):
        name = vert_ref[h, k]
        gap = mine - name
        ok = gap > 0
        for n in range(8):
            ok = ok & (slash_ref[h, n] != gap)
        bias.append(jnp.where(ok, 0.0, NEG).astype(F32))
        places.append(pos_ref[h, k])
    scores = []
    for k in range(0, 8, 2):
        both = dot(q, jnp.concatenate([far_ref[places[k], 0], far_ref[places[k + 1], 0]], axis=1))
        scores.append(both[:, :BLK] + bias[k])
        scores.append(both[:, BLK:] + bias[k + 1])
    old = top_ref[h, rows, :]
    top = jnp.maximum(old, lane_max(scores))
    keep = jnp.exp2((old - top) * SCALE2)
    weights = [jnp.exp2((s - top) * SCALE2) for s in scores]
    acc = None
    for k in range(0, 8, 2):
        p = jnp.concatenate([weights[k].astype(BF16), weights[k + 1].astype(BF16)], axis=1)
        v = jnp.concatenate([far_ref[places[k], 1], far_ref[places[k + 1], 1]], axis=0)
        acc = dot(p, v) if acc is None else acc + dot(p, v)
    total = sum_ref[h, rows, :] * keep + lane_sum(weights)
    out_ref[h, rows, :] = ((acc_ref[h, rows, :] * keep + acc) / total).astype(BF16)


CAP = 4
SEQ = ("seq_0", "seq_1", "seq_2")
SEQ_HEAD = ("seq_0", "seq_1", "seq_2", "head")
UNROLL = 4


def joined_along(blocks, dim):
    dims = list(blocks.shape[1:])
    dims[dim] *= blocks.shape[0]
    return jnp.moveaxis(blocks, 0, dim).reshape(dims)


def stacked_from(array, axes, order):
    blocks = array
    for k in order:
        blocks = lax.all_gather(blocks, axes[k])
    done = order[::-1]
    back = [done.index(k) for k in range(len(axes))]
    blocks = blocks.transpose(*back, *range(len(axes), blocks.ndim))
    return blocks.reshape(-1, *array.shape)


def whole_of(array, axes, order, dim):
    return joined_along(stacked_from(array, axes, order), dim)


def shifted(array, axis, by):
    peers = lax.axis_size(axis)
    pairs = [(i, i + by) for i in range(peers) if 0 <= i + by < peers]
    return lax.ppermute(array, axis, pairs)


def kernel(slab_ref, slash, vert, pos, q_hbm, ext_hbm, far_hbm, out_hbm, q, ext, far, acc, top, tot, out, sem):
    loads = [
        pltpu.make_async_copy(q_hbm.at[:, pl.ds(h * 128, 128)], q.at[h], sem.at[h]) for h in range(8)
    ]
    loads.append(pltpu.make_async_copy(ext_hbm, ext, sem.at[8]))
    late = pltpu.make_async_copy(far_hbm, far, sem.at[9])
    for load in loads:
        load.start()
    late.start()
    for load in loads:
        load.wait()
    slab = slab_ref[0]

    @pl.loop(0, 64 // UNROLL)
    def _(t):
        for u in range(UNROLL):
            e = t * UNROLL + u
            near_step(e // 8, e % 8, slab, slash, q, ext, acc, top, tot)

    late.wait()

    @pl.loop(0, 64 // UNROLL)
    def _(t):
        for u in range(UNROLL):
            e = t * UNROLL + u
            far_step(e // 8, e % 8, slab, slash, vert, pos, q, far, acc, top, tot, out)

    stores = [
        pltpu.make_async_copy(out.at[h], out_hbm.at[:, pl.ds(h * 128, 128)], sem.at[h]) for h in range(8)
    ]
    for store in stores:
        store.start()
    for store in stores:
        store.wait()


def attention(slab, slash, vert, pos, q, ext, far):
    whole = pl.BlockSpec(memory_space=pl.ANY)
    scalars = pl.BlockSpec(memory_space=pltpu.SMEM)
    return pl.pallas_call(
        kernel,
        out_shape=jax.ShapeDtypeStruct((1024, 1024), BF16),
        in_specs=[scalars] * 4 + [whole] * 3,
        out_specs=whole,
        scratch_shapes=[
            pltpu.VMEM((8, 1024, 128), BF16),
            pltpu.VMEM((36, 2, 128, 128), BF16),
            pltpu.VMEM((128, 2, 128, 128), BF16),
            pltpu.VMEM((8, 1024, 128), F32),
            pltpu.VMEM((8, 1024, 1), F32),
            pltpu.VMEM((8, 1024, 1), F32),
            pltpu.VMEM((8, 1024, 128), BF16),
            pltpu.SemaphoreType.DMA((10,)),
        ],
        compiler_params=pltpu.CompilerParams(vmem_limit_bytes=60 * 2**20),
    )(slab, slash, vert, pos, q, ext, far)


def shards(queries, keys, values, vertical, slash):
    slab = lax.axis_index(SEQ)
    local_kv = jnp.stack(
        [keys.reshape(8, BLK, BLK).transpose(0, 2, 1), values.reshape(8, BLK, BLK)], axis=1
    )
    flat = vertical.reshape(-1)
    used = jnp.any(flat[:, None] == jnp.arange(256, dtype=jnp.int32)[None, :], axis=0)
    ids = jnp.arange(256, dtype=jnp.int32)
    earlier = used[None, :] & (ids[None, :] // 8 == flat[:, None] // 8) & (ids[None, :] < flat[:, None])
    pos = (flat // 8) * CAP + jnp.sum(earlier.astype(jnp.int32), axis=1)
    mine = lax.dynamic_slice_in_dim(used, slab * 8, 8)
    ranks = jnp.cumsum(mine.astype(jnp.int32)) - 1
    select = mine[None, :] & (ranks[None, :] == jnp.arange(CAP, dtype=jnp.int32)[:, None])
    which = jnp.sum(jnp.where(select, jnp.arange(8, dtype=jnp.int32)[None, :], 0), axis=1)
    packed = jnp.take(local_kv, which, axis=0)
    far = whole_of(packed, SEQ, (2, 0, 1), 0)
    ext = jnp.concatenate([shifted(local_kv, SEQ, k)[(4 if k == 4 else 0):] for k in (4, 3, 2, 1)] + [local_kv], axis=0)
    attended = attention(slab.reshape(1), slash, vertical, pos.reshape(8, 8), queries, ext, far)
    return lax.all_to_all(attended, "head", split_axis=0, concat_axis=1, tiled=True)


def solution(mesh):
    split = Mesh(
        mesh.devices.reshape(mesh.shape["head"], 4, 4, 2), ("head", "seq_0", "seq_1", "seq_2")
    )
    return jax.shard_map(
        shards,
        mesh=split,
        in_specs=(P(SEQ, "head"), P(SEQ, "head"), P(SEQ, "head"), P("head", None), P("head", None)),
        out_specs=P(SEQ_HEAD, None),
        check_vma=False,
    )
```

```python
import functools, math
import jax, jax.numpy as jnp
from jax import lax
from jax.experimental import pallas as pl
from jax.experimental.pallas import tpu as pltpu
from jax.sharding import PartitionSpec as P

BLK = 128
NEG = -1e30
BACK = 28
F32 = jnp.float32
BF16 = jnp.bfloat16
SCALE2 = math.log2(math.e) / math.sqrt(128.0)


def dot(a, b):
    return jnp.dot(a, b, preferred_element_type=F32)


def lane_max(parts):
    top = parts[0]
    for part in parts[1:]:
        top = jnp.maximum(top, part)
    return jnp.max(top, axis=1, keepdims=True)


def lane_sum(parts):
    total = parts[0]
    for part in parts[1:]:
        total = total + part
    return jnp.sum(total, axis=1, keepdims=True)


def near_step(h, i, slab, slash_ref, q_ref, ext_ref, acc_ref, top_ref, sum_ref):
    rows = pl.ds(pl.multiple_of(i * BLK, BLK), BLK)
    q = q_ref[h, rows, :]
    row = lax.broadcasted_iota(jnp.int32, (BLK, BLK), 0)
    col = lax.broadcasted_iota(jnp.int32, (BLK, BLK), 1)
    own = BACK + i
    scores = [jnp.where(row >= col, dot(q, ext_ref[own, 0]), NEG)]
    blocks = [own]
    for n in range(0, 8, 2):
        pair, bias = [], []
        for k in (n, n + 1):
            off = slash_ref[h, k]
            ok = slab * 8 + i - off >= 0
            pair.append(jnp.where(ok, own - off, own))
            bias.append(jnp.where(ok, 0.0, NEG).astype(F32))
        both = dot(q, jnp.concatenate([ext_ref[pair[0], 0], ext_ref[pair[1], 0]], axis=1))
        scores.append(both[:, :BLK] + bias[0])
        scores.append(both[:, BLK:] + bias[1])
        blocks += pair
    top = lane_max(scores)
    weights = [jnp.exp2((s - top) * SCALE2) for s in scores]
    acc = dot(weights[0].astype(BF16), ext_ref[blocks[0], 1])
    for n in range(1, 9, 2):
        p = jnp.concatenate([weights[n].astype(BF16), weights[n + 1].astype(BF16)], axis=1)
        v = jnp.concatenate([ext_ref[blocks[n], 1], ext_ref[blocks[n + 1], 1]], axis=0)
        acc = acc + dot(p, v)
    acc_ref[h, rows, :] = acc
    top_ref[h, rows, :] = top
    sum_ref[h, rows, :] = lane_sum(weights)


def far_step(h, i, slab, slash_ref, vert_ref, pos_ref, q_ref, far_ref, acc_ref, top_ref, sum_ref, out_ref):
    rows = pl.ds(pl.multiple_of(i * BLK, BLK), BLK)
    q = q_ref[h, rows, :]
    mine = slab * 8 + i
    bias, places = [], []
    for k in range(8):
        name = vert_ref[h, k]
        gap = mine - name
        ok = gap > 0
        for n in range(8):
            ok = ok & (slash_ref[h, n] != gap)
        bias.append(jnp.where(ok, 0.0, NEG).astype(F32))
        places.append((pos_ref[h, k], pos_ref[8 + h, k]))
    scores = []
    for k in range(0, 8, 2):
        both = dot(q, jnp.concatenate([far_ref[places[k][0], places[k][1]], far_ref[places[k + 1][0], places[k + 1][1]]], axis=1))
        scores.append(both[:, :BLK] + bias[k])
        scores.append(both[:, BLK:] + bias[k + 1])
    old = top_ref[h, rows, :]
    top = jnp.maximum(old, lane_max(scores))
    keep = jnp.exp2((old - top) * SCALE2)
    weights = [jnp.exp2((s - top) * SCALE2) for s in scores]
    acc = None
    for k in range(0, 8, 2):
        p = jnp.concatenate([weights[k].astype(BF16), weights[k + 1].astype(BF16)], axis=1)
        v = jnp.concatenate([far_ref[places[k][0], places[k][1] + 1], far_ref[places[k + 1][0], places[k + 1][1] + 1]], axis=0)
        acc = dot(p, v) if acc is None else acc + dot(p, v)
    total = sum_ref[h, rows, :] * keep + lane_sum(weights)
    out_ref[h, rows, :] = ((acc_ref[h, rows, :] * keep + acc) / total).astype(BF16)


MESH = pl.DeviceIdType.MESH
UNROLL = 4
DIRS = (1, -1)
NAMES = ["y", "zP-", "zP+", "zP2", "hA", "hB", "h3", "h4", "y1", "y2", "y3"]
NAMES += [kind + str(d) for kind in ("xo", "xp", "x1", "x2", "x3", "ro", "r1", "r2", "r3") for d in DIRS]
NAMES += ["R" + str(j) + str(d) for j in (0, 1, -1, 2) for d in DIRS]
NAMES += ["RR" + str(j) for j in (0, 1, -1, 2)]
INDEX = {name: n for n, name in enumerate(NAMES)}


def kernel(slash, vert, place, which, q_hbm, k_hbm, v_hbm, out_hbm,
           q, raw, own, ext, far, acc, top, tot, out, load_sem, send_sem, recv_sem, part_sem, part_recv, keep_sem):
    group = lax.axis_index("head")
    slab = lax.axis_index("seq")
    x, z, half = slab // 8, (slab // 2) % 4, slab % 2
    loads = [
        pltpu.make_async_copy(k_hbm, raw, load_sem.at[8]),
        pltpu.make_async_copy(v_hbm, own.at[:, 1], load_sem.at[9]),
        pltpu.make_async_copy(v_hbm, ext.at[pl.ds(BACK, 8), 1], load_sem.at[10]),
    ]
    heads = [
        pltpu.make_async_copy(q_hbm.at[:, pl.ds(h * BLK, BLK)], q.at[h], load_sem.at[h]) for h in range(8)
    ]
    for load in loads + heads:
        load.start()

    def seat(dx, dz, dy):
        return ((x + dx) % 4) * 8 + ((z + dz) % 4) * 2 + ((half + dy) % 2)

    def spot(g, s):
        return (g, s)

    mate = spot(group, seat(0, 0, 1))
    after = spot(group, (slab + 2) % 32)
    before = spot(group, (slab + 30) % 32)
    across = {d: spot(group, seat(d, 0, 0)) for d in DIRS}
    along = {d: spot(group, seat(0, d, 0)) for d in DIRS}
    peers = [spot((group + n) % 4, slab) for n in (1, 2, 3)]
    barrier = pltpu.get_barrier_semaphore()
    friends = [mate, after, before, across[1], across[-1], along[1], along[-1]] + peers
    for friend in friends:
        pl.semaphore_signal(barrier, inc=1, device_id=friend, device_id_type=MESH)

    for load in loads:
        load.wait()
    for b in range(8):
        flipped = raw[b].astype(F32).T.astype(BF16)
        own[b, 0] = flipped
        ext[BACK + b, 0] = flipped
    for c in range(4):
        far[slab, 2 * c] = own[which[0, c], 0]
        far[slab, 2 * c + 1] = own[which[0, c], 1]
    pl.semaphore_wait(barrier, len(friends))

    PP, RR, ALL = (0, 5), (5, 3), (0, 8)

    def one(dx, dz, side, sub):
        return far.at[pl.ds(((x + dx) % 4) * 8 + ((z + dz) % 4) * 2 + side, 1), pl.ds(*sub)]

    def pair(dx, dz, sub):
        return far.at[pl.ds(((x + dx) % 4) * 8 + ((z + dz) % 4) * 2, 2), pl.ds(*sub)]

    def near(at, side_step=0):
        return ext.at[pl.ds(at + side_step * half, 4)]

    plan = {
        "y": (one(0, 0, half, ALL), None, mate, one(0, 0, 1 - half, ALL)),
        "zP-": (pair(0, 0, PP), None, along[-1], pair(0, 1, PP)),
        "zP+": (pair(0, 0, PP), None, along[1], pair(0, -1, PP)),
        "zP2": (pair(0, 1, PP), None, along[-1], pair(0, 2, PP)),
        "hA": (near(28), near(12), after, near(12)),
        "hB": (near(32), near(16), after, near(16)),
        "h4": (near(16), near(0), after, near(0)),
        "h3": (near(20), near(4), after, near(4)),
        "y1": (near(28, -16), near(20), mate, near(20)),
        "y2": (near(32, -16), near(24), mate, near(24)),
        "y3": (near(16, -16), near(8), mate, near(8)),
    }
    for d in DIRS:
        side = 0 if d == 1 else 1
        plan["xo" + str(d)] = (one(0, 0, half, ALL), None, across[d], one(-d, 0, half, ALL))
        plan["xp" + str(d)] = (one(0, 0, 1 - half, ALL), None, across[d], one(-d, 0, 1 - half, ALL))
        plan["ro" + str(d)] = (one(-d, 0, side, ALL), None, across[d], one(2, 0, side, ALL))
        for n, dz in (("1", 1), ("2", 2), ("3", -1)):
            plan["x" + n + str(d)] = (pair(0, dz, PP), None, across[d], pair(-d, dz, PP))
            plan["r" + n + str(d)] = (one(-d, dz, side, PP), None, across[d], one(2, dz, side, PP))
        for j in (0, 1, -1, 2):
            plan["R" + str(j) + str(d)] = (pair(j, 0, RR), None, along[d], pair(j, -d, RR))
    for j in (0, 1, -1, 2):
        d = 1 if j == 2 else -1
        plan["RR" + str(j)] = (pair(j, -d, RR), None, along[d], pair(j, 2, RR))

    def copy(name, landing):
        source, target, device, lands = plan[name]
        n = INDEX[name]
        return pltpu.make_async_remote_copy(
            src_ref=lands if landing else source,
            dst_ref=lands if landing else (source if target is None else target),
            send_sem=send_sem.at[n],
            recv_sem=recv_sem.at[n],
            device_id=device,
            device_id_type=MESH,
        )

    def send(*names):
        for name in names:
            copy(name, False).start()

    waited = []

    def take(*names):
        for name in names:
            copy(name, True).wait_recv()
            waited.append(name)

    send("y", "xo1", "xo-1", "hA", "hB")
    take("hA")
    send("y1")
    take("y")
    send("xp1", "xp-1", "zP-")
    take("hB")
    send("y2", "h4")
    take("y1")
    send("h3", "zP+")
    take("xo1", "xo-1", "xp1", "xp-1")
    send("ro1", "ro-1")
    take("zP-")
    send("zP2", "x11", "x1-1", "R01", "R0-1", "R11", "R1-1", "R-11", "R-1-1")
    take("h4")
    send("y3")
    take("ro1", "ro-1")
    send("R21", "R2-1")
    take("zP2")
    send("x21", "x2-1")
    for head in heads:
        head.wait()
    take("y2", "h3", "y3")

    def at_1():
        take("x11", "x1-1")
        send("r11", "r1-1")

    def at_3():
        take("zP+")
        send("x31", "x3-1")

    def at_6():
        take("R0-1", "R1-1", "R-1-1")
        send("RR0", "RR1", "RR-1")

    def at_8():
        take("x21", "x2-1")
        send("r21", "r2-1")

    def at_10():
        take("R21")
        send("RR2")

    def at_13():
        take("x31", "x3-1")
        send("r31", "r3-1")

    events = {1: at_1, 3: at_3, 6: at_6, 8: at_8, 10: at_10, 13: at_13}

    @pl.loop(0, 64 // UNROLL)
    def _(t):
        for when, event in events.items():
            pl.when(t == when)(event)
        for u in range(UNROLL):
            e = t * UNROLL + u
            near_step(e // 8, e % 8, slab, slash, q, ext, acc, top, tot)

    take(*[name for name in NAMES if name not in waited])

    def quarter(h, n):
        return out.at[h, pl.ds(((group + n) % 4) * 256, 256)]

    def column(h):
        return out_hbm.at[:, pl.ds(pl.multiple_of((group * 8 + h) * BLK, BLK), BLK)]

    def share(h, n):
        return pltpu.make_async_remote_copy(
            src_ref=quarter(h, n),
            dst_ref=column(h),
            send_sem=part_sem.at[h, n - 1],
            recv_sem=part_recv.at[h, n - 1],
            device_id=peers[n - 1],
            device_id_type=MESH,
        )

    def keep(h):
        return pltpu.make_async_copy(quarter(h, 0), column(h), keep_sem.at[h])

    @pl.loop(0, 8)
    def _(h):
        @pl.loop(0, 8 // UNROLL)
        def _(t):
            for u in range(UNROLL):
                far_step(h, t * UNROLL + u, slab, slash, vert, place, q, far, acc, top, tot, out)

        for n in (2, 1, 3):
            share(h, n).start()
        keep(h).start()

    for name in NAMES:
        copy(name, False).wait_send()

    @pl.loop(0, 8)
    def _(h):
        keep(h).wait()
        for n in (1, 2, 3):
            origin = (group - n + 4) % 4
            share(h, n).wait_send()
            lands = out_hbm.at[:, pl.ds(pl.multiple_of((origin * 8 + h) * BLK, BLK), BLK)]
            pltpu.make_async_remote_copy(
                src_ref=quarter(h, n),
                dst_ref=lands,
                send_sem=part_sem.at[h, n - 1],
                recv_sem=part_recv.at[h, n - 1],
                device_id=peers[n - 1],
                device_id_type=MESH,
            ).wait_recv()


def attention(slash, vert, place, which, q, k, v):
    whole = pl.BlockSpec(memory_space=pl.ANY)
    scalars = pl.BlockSpec(memory_space=pltpu.SMEM)
    return pl.pallas_call(
        kernel,
        out_shape=jax.ShapeDtypeStruct((256, 4096), BF16),
        in_specs=[scalars] * 4 + [whole] * 3,
        out_specs=whole,
        scratch_shapes=[
            pltpu.VMEM((8, 1024, 128), BF16),
            pltpu.VMEM((8, 128, 128), BF16),
            pltpu.VMEM((8, 2, 128, 128), BF16),
            pltpu.VMEM((36, 2, 128, 128), BF16),
            pltpu.VMEM((32, 8, 128, 128), BF16),
            pltpu.VMEM((8, 1024, 128), F32),
            pltpu.VMEM((8, 1024, 1), F32),
            pltpu.VMEM((8, 1024, 1), F32),
            pltpu.VMEM((8, 1024, 128), BF16),
            pltpu.SemaphoreType.DMA((11,)),
            pltpu.SemaphoreType.DMA((len(NAMES),)),
            pltpu.SemaphoreType.DMA((len(NAMES),)),
            pltpu.SemaphoreType.DMA((8, 3)),
            pltpu.SemaphoreType.DMA((8, 3)),
            pltpu.SemaphoreType.DMA((8,)),
        ],
        compiler_params=pltpu.CompilerParams(
            collective_id=0, has_side_effects=True, vmem_limit_bytes=60 * 2**20
        ),
    )(slash, vert, place, which, q, k, v)


def shards(queries, keys, values, vertical, slash):
    slab = lax.axis_index("seq")
    ids = jnp.arange(256, dtype=jnp.int32)
    flat = vertical.reshape(-1)
    used = jnp.any(flat[:, None] == ids[None, :], axis=0)
    earlier = used[None, :] & (ids[None, :] // 8 == flat[:, None] // 8) & (ids[None, :] < flat[:, None])
    rank = jnp.sum(earlier.astype(jnp.int32), axis=1)
    place = jnp.concatenate([vertical // 8, 2 * rank.reshape(8, 8)], axis=0)
    mine = flat[:, None] - slab * 8
    slots = jnp.arange(4, dtype=jnp.int32)[None, :]
    hit = (mine >= 0) & (mine < 8) & (rank[:, None] == slots)
    which = jnp.max(jnp.where(hit, mine, 0), axis=0, keepdims=True)
    return attention(
        slash, vertical, place, which, queries, keys.reshape(8, BLK, BLK), values.reshape(8, BLK, BLK)
    )


def solution(mesh):
    return jax.shard_map(
        shards,
        mesh=mesh,
        in_specs=(P("seq", "head"), P("seq", "head"), P("seq", "head"), P("head", None), P("head", None)),
        out_specs=P(("seq", "head"), None),
        check_vma=False,
    )
```

```python
import functools, math
import jax, jax.numpy as jnp
from jax import lax
from jax.experimental import pallas as pl
from jax.experimental.pallas import tpu as pltpu
from jax.sharding import PartitionSpec as P

BLK = 128
NEG = -1e30
BACK = 28
F32 = jnp.float32
BF16 = jnp.bfloat16
SCALE2 = math.log2(math.e) / math.sqrt(128.0)


def dot(a, b):
    return jnp.dot(a, b, preferred_element_type=F32)


def lane_max(parts):
    top = parts[0]
    for part in parts[1:]:
        top = jnp.maximum(top, part)
    return jnp.max(top, axis=1, keepdims=True)


def lane_sum(parts):
    total = parts[0]
    for part in parts[1:]:
        total = total + part
    return jnp.sum(total, axis=1, keepdims=True)


def cat_dot(ps, vs):
    return dot(jnp.concatenate([p.astype(BF16) for p in ps], axis=1), jnp.concatenate(vs, axis=0))

def near_scores(h, i, slab, slash_ref, q_ref, ext_ref):
    rows = pl.ds(pl.multiple_of(i * BLK, BLK), BLK)
    q = q_ref[h, rows, :]
    row = lax.broadcasted_iota(jnp.int32, (BLK, BLK), 0)
    col = lax.broadcasted_iota(jnp.int32, (BLK, BLK), 1)
    own = BACK + i
    blocks = [own]
    bias = []
    for k in range(8):
        off = slash_ref[h, k]
        ok = slab * 8 + i - off >= 0
        blocks.append(jnp.where(ok, own - off, own))
        bias.append(jnp.where(ok, 0.0, NEG).astype(F32))
    scores = [jnp.where(row >= col, dot(q, ext_ref[own, 0]), NEG)]
    for k in range(0, 8, 2):
        both = dot(q, jnp.concatenate([ext_ref[blocks[1 + k], 0], ext_ref[blocks[2 + k], 0]], axis=1))
        scores.append(both[:, :BLK] + bias[k])
        scores.append(both[:, BLK:] + bias[k + 1])
    return scores, blocks, rows

def far_scores(h, i, slab, slash_ref, vert_ref, pos_ref, q_ref, far_ref):
    rows = pl.ds(pl.multiple_of(i * BLK, BLK), BLK)
    q = q_ref[h, rows, :]
    mine = slab * 8 + i
    bias, places = [], []
    for k in range(8):
        gap = mine - vert_ref[h, k]
        ok = gap > 0
        for n in range(8):
            ok = ok & (slash_ref[h, n] != gap)
        bias.append(jnp.where(ok, 0.0, NEG).astype(F32))
        places.append((jnp.where(ok, pos_ref[h, k], slab), jnp.where(ok, pos_ref[8 + h, k], 0)))
    scores = []
    for k in range(0, 8, 2):
        both = dot(q, jnp.concatenate([far_ref[places[k][0], places[k][1]], far_ref[places[k + 1][0], places[k + 1][1]]], axis=1))
        scores.append(both[:, :BLK] + bias[k])
        scores.append(both[:, BLK:] + bias[k + 1])
    return scores, places, rows

def near_put(slot, e, slab, slash, q, ext, stage):
    scores, _, _ = near_scores(e // 8, e % 8, slab, slash, q, ext)
    for k, s in enumerate(scores):
        stage[slot, k] = s


def near_finish(slot, e, slab, slash, ext, acc, top, tot, stage):
    h, i = e // 8, e % 8
    rows = pl.ds(pl.multiple_of(i * BLK, BLK), BLK)
    own = BACK + i
    blocks = [own]
    for k in range(8):
        off = slash[h, k]
        blocks.append(jnp.where(slab * 8 + i - off >= 0, own - off, own))
    scores = [stage[slot, k] for k in range(9)]
    best = lane_max(scores)
    weights = [jnp.exp2((s - best) * SCALE2) for s in scores]
    acc[h, rows, :] = cat_dot(weights, [ext[b, 1] for b in blocks])
    top[h, rows, :] = best
    tot[h, rows, :] = lane_sum(weights)


def far_put(slot, e, slab, slash, vert, pos, q, far, stage, spots):
    scores, places, _ = far_scores(e // 8, e % 8, slab, slash, vert, pos, q, far)
    for k, s in enumerate(scores):
        stage[slot, k] = s
        spots[slot, k] = places[k][0]
        spots[slot, 8 + k] = places[k][1]


def far_finish(slot, e, far, acc, top, tot, out, stage, spots):
    h, i = e // 8, e % 8
    rows = pl.ds(pl.multiple_of(i * BLK, BLK), BLK)
    scores = [stage[slot, k] for k in range(8)]
    old = top[h, rows, :]
    best = jnp.maximum(old, lane_max(scores))
    keep = jnp.exp2((old - best) * SCALE2)
    weights = [jnp.exp2((s - best) * SCALE2) for s in scores]
    mixed = cat_dot(weights, [far[spots[slot, k], spots[slot, 8 + k] + 1] for k in range(8)])
    total = tot[h, rows, :] * keep + lane_sum(weights)
    out[h, rows, :] = ((acc[h, rows, :] * keep + mixed) / total).astype(BF16)


MESH = pl.DeviceIdType.MESH
NEAR_STEPS = 4
FAR_STEPS = 4
DIRS = (1, -1)
NAMES = ["y", "zP-", "zP+", "zP2", "hA", "hB", "h3", "h4", "y1", "y2", "y3"]
NAMES += [kind + str(d) for kind in ("xo", "xp", "x1", "x2", "x3") for d in DIRS]
NAMES += ["ro", "rp", "r1", "r2", "r3"]
NAMES += ["R" + str(j) + str(d) for j in (0, 1, 2, 3) for d in DIRS]
NAMES += ["RR" + str(j) for j in (0, 1, 2, 3)]
INDEX = {name: n for n, name in enumerate(NAMES)}


def kernel(slash, vert, place, which, q_hbm, k_hbm, v_hbm, out_hbm,
           q, raw, own, ext, far, acc, top, tot, out, stage, spots, load_sem, send_sem, recv_sem, part_sem, part_recv, keep_sem):
    group = lax.axis_index("head")
    slab = lax.axis_index("seq")
    x, z, half = slab // 8, (slab // 2) % 4, slab % 2
    loads = [
        pltpu.make_async_copy(k_hbm, raw, load_sem.at[8]),
        pltpu.make_async_copy(v_hbm, own.at[:, 1], load_sem.at[9]),
        pltpu.make_async_copy(v_hbm, ext.at[pl.ds(BACK, 8), 1], load_sem.at[10]),
    ]
    heads = [
        pltpu.make_async_copy(q_hbm.at[:, pl.ds(h * BLK, BLK)], q.at[h], load_sem.at[h]) for h in range(8)
    ]
    for load in loads + heads:
        load.start()

    def seat(dx, dz, dy):
        return ((x + dx) % 4) * 8 + ((z + dz) % 4) * 2 + ((half + dy) % 2)

    def spot(g, s):
        return (g, s)

    mate = spot(group, seat(0, 0, 1))
    after = spot(group, (slab + 2) % 32)
    before = spot(group, (slab + 30) % 32)
    across = {d: spot(group, seat(d, 0, 0)) for d in DIRS}
    along = {d: spot(group, seat(0, d, 0)) for d in DIRS}
    peers = [spot((group + n) % 4, slab) for n in (1, 2, 3)]
    barrier = pltpu.get_barrier_semaphore()
    friends = [mate, after, before, across[1], across[-1], along[1], along[-1]] + peers
    for friend in friends:
        pl.semaphore_signal(barrier, inc=1, device_id=friend, device_id_type=MESH)

    for load in loads:
        load.wait()
    for b in range(8):
        flipped = raw[b].astype(F32).T.astype(BF16)
        own[b, 0] = flipped
        ext[BACK + b, 0] = flipped
    for c in range(4):
        far[slab, 2 * c] = own[which[0, c], 0]
        far[slab, 2 * c + 1] = own[which[0, c], 1]
    pl.semaphore_wait(barrier, len(friends))

    PP, RR, ALL = (0, 4), (4, 4), (0, 8)

    def one(dx, dz, side, sub):
        return far.at[pl.ds(((x + dx) % 4) * 8 + ((z + dz) % 4) * 2 + side, 1), pl.ds(*sub)]

    def pair(dx, dz, sub):
        return far.at[pl.ds(((x + dx) % 4) * 8 + ((z + dz) % 4) * 2, 2), pl.ds(*sub)]

    def near(at, side_step=0):
        return ext.at[pl.ds(at + side_step * half, 4)]

    plan = {
        "y": (one(0, 0, half, ALL), None, mate, one(0, 0, 1 - half, ALL)),
        "zP-": (pair(0, 0, PP), None, along[-1], pair(0, 1, PP)),
        "zP+": (pair(0, 0, PP), None, along[1], pair(0, -1, PP)),
        "zP2": (pair(0, 1, PP), None, along[-1], pair(0, 2, PP)),
        "hA": (near(28), near(12), after, near(12)),
        "hB": (near(32), near(16), after, near(16)),
        "h4": (near(16), near(0), after, near(0)),
        "h3": (near(20), near(4), after, near(4)),
        "y1": (near(28, -16), near(20), mate, near(20)),
        "y2": (near(32, -16), near(24), mate, near(24)),
        "y3": (near(16, -16), near(8), mate, near(8)),
    }
    sends = {d: x < 3 if d == 1 else x < 2 for d in DIRS}
    takes = {d: x > 0 if d == 1 else (x == 3) | (x == 0) for d in DIRS}
    sender, taker = {}, {}
    for d in DIRS:
        for n, source, lands in (
            ("xo", one(0, 0, half, ALL), one(-d, 0, half, ALL)),
            ("xp", one(0, 0, 1 - half, ALL), one(-d, 0, 1 - half, ALL)),
            ("x1", pair(0, 1, PP), pair(-d, 1, PP)),
            ("x2", pair(0, 2, PP), pair(-d, 2, PP)),
            ("x3", pair(0, -1, PP), pair(-d, -1, PP)),
        ):
            plan[n + str(d)] = (source, None, across[d], lands)
            sender[n + str(d)] = sends[d]
            taker[n + str(d)] = takes[d]
        for j in (0, 1, 2, 3):
            plan["R" + str(j) + str(d)] = (pair(-j, 0, RR), None, along[d], pair(-j, -d, RR))
            if j:
                sender["R" + str(j) + str(d)] = taker["R" + str(j) + str(d)] = x >= j
    for n, source, lands in (
        ("ro", one(1, 0, half, ALL), one(2, 0, half, ALL)),
        ("rp", one(1, 0, 1 - half, ALL), one(2, 0, 1 - half, ALL)),
        ("r1", pair(1, 1, PP), pair(2, 1, PP)),
        ("r2", pair(1, 2, PP), pair(2, 2, PP)),
        ("r3", pair(1, -1, PP), pair(2, -1, PP)),
    ):
        plan[n] = (source, None, across[-1], lands)
        sender[n] = (x == 0) | (x == 3)
        taker[n] = (x == 3) | (x == 2)
    for j in (0, 1, 2, 3):
        d = 1 if j == 2 else -1
        plan["RR" + str(j)] = (pair(-j, -d, RR), None, along[d], pair(-j, 2, RR))
        if j:
            sender["RR" + str(j)] = taker["RR" + str(j)] = x >= j

    def copy(name, landing):
        source, target, device, lands = plan[name]
        n = INDEX[name]
        return pltpu.make_async_remote_copy(
            src_ref=lands if landing else source,
            dst_ref=lands if landing else (source if target is None else target),
            send_sem=send_sem.at[n],
            recv_sem=recv_sem.at[n],
            device_id=device,
            device_id_type=MESH,
        )

    def guarded(rule, name, act):
        if name in rule:
            pl.when(rule[name])(act)
        else:
            act()

    def send(*names):
        for name in names:
            guarded(sender, name, lambda name=name: copy(name, False).start())

    waited = []

    def take(*names):
        for name in names:
            guarded(taker, name, lambda name=name: copy(name, True).wait_recv())
            waited.append(name)

    send("y", "xo1", "xo-1", "hA", "hB")
    take("hA")
    send("y1")
    take("y")
    send("xp1", "xp-1", "zP-")
    take("hB")
    send("y2", "h4")
    take("y1")
    send("h3", "zP+")
    take("xo1", "xo-1", "xp1", "xp-1")
    send("ro", "rp")
    take("zP-")
    send("zP2", "x11", "x1-1", "R11", "R1-1", "R01", "R0-1")
    take("h4")
    send("y3")
    take("zP2")
    send("x21", "x2-1")
    for head in heads:
        head.wait()
    take("y2", "h3", "y3")

    def at_1():
        take("x11", "x1-1")
        send("r1")

    def at_2():
        take("zP+")
        send("x31", "x3-1")

    def at_3():
        take("ro", "rp")
        send("R31", "R3-1", "R21", "R2-1")

    def at_5():
        take("R0-1", "R1-1")
        send("RR0", "RR1")

    def at_7():
        take("x21", "x2-1")
        send("r2")

    def at_9():
        take("R3-1", "R21")
        send("RR3", "RR2")

    def at_12():
        take("x31", "x3-1")
        send("r3")

    events = {2: at_1, 5: at_2, 7: at_3, 10: at_5}
    near_put(0, 0, slab, slash, q, ext, stage)

    @pl.loop(0, 64 // NEAR_STEPS)
    def _(t):
        for when, event in events.items():
            pl.when(t == when)(event)
        for u in range(NEAR_STEPS):
            e = t * NEAR_STEPS + u
            near_put((u + 1) % 2, jnp.minimum(e + 1, 63), slab, slash, q, ext, stage)
            near_finish(u % 2, e, slab, slash, ext, acc, top, tot, stage)

    at_7()
    at_9()
    at_12()
    take(*[name for name in NAMES if name not in waited])

    def quarter(h, n):
        return out.at[h, pl.ds(((group + n) % 4) * 256, 256)]

    def column(h):
        return out_hbm.at[:, pl.ds(pl.multiple_of((group * 8 + h) * BLK, BLK), BLK)]

    def share(h, n):
        return pltpu.make_async_remote_copy(
            src_ref=quarter(h, n),
            dst_ref=column(h),
            send_sem=part_sem.at[h, n - 1],
            recv_sem=part_recv.at[h, n - 1],
            device_id=peers[n - 1],
            device_id_type=MESH,
        )

    def keep(h):
        return pltpu.make_async_copy(quarter(h, 0), column(h), keep_sem.at[h])

    far_put(0, 0, slab, slash, vert, place, q, far, stage, spots)

    @pl.loop(0, 8)
    def _(h):
        @pl.loop(0, 8 // FAR_STEPS)
        def _(t):
            for u in range(FAR_STEPS):
                e = h * 8 + t * FAR_STEPS + u
                far_put((u + 1) % 2, jnp.minimum(e + 1, 63), slab, slash, vert, place, q, far, stage, spots)
                far_finish(u % 2, e, far, acc, top, tot, out, stage, spots)

        for n in (2, 1, 3):
            share(h, n).start()
        keep(h).start()

    for name in NAMES:
        guarded(sender, name, lambda name=name: copy(name, False).wait_send())

    @pl.loop(0, 8)
    def _(h):
        keep(h).wait()
        for n in (1, 2, 3):
            origin = (group - n + 4) % 4
            share(h, n).wait_send()
            lands = out_hbm.at[:, pl.ds(pl.multiple_of((origin * 8 + h) * BLK, BLK), BLK)]
            pltpu.make_async_remote_copy(
                src_ref=quarter(h, n),
                dst_ref=lands,
                send_sem=part_sem.at[h, n - 1],
                recv_sem=part_recv.at[h, n - 1],
                device_id=peers[n - 1],
                device_id_type=MESH,
            ).wait_recv()


def attention(slash, vert, place, which, q, k, v):
    whole = pl.BlockSpec(memory_space=pl.ANY)
    scalars = pl.BlockSpec(memory_space=pltpu.SMEM)
    return pl.pallas_call(
        kernel,
        out_shape=jax.ShapeDtypeStruct((256, 4096), BF16),
        in_specs=[scalars] * 4 + [whole] * 3,
        out_specs=whole,
        scratch_shapes=[
            pltpu.VMEM((8, 1024, 128), BF16),
            pltpu.VMEM((8, 128, 128), BF16),
            pltpu.VMEM((8, 2, 128, 128), BF16),
            pltpu.VMEM((36, 2, 128, 128), BF16),
            pltpu.VMEM((32, 8, 128, 128), BF16),
            pltpu.VMEM((8, 1024, 128), F32),
            pltpu.VMEM((8, 1024, 1), F32),
            pltpu.VMEM((8, 1024, 1), F32),
            pltpu.VMEM((8, 1024, 128), BF16),
            pltpu.VMEM((2, 9, 128, 128), F32),
            pltpu.SMEM((2, 16), jnp.int32),
            pltpu.SemaphoreType.DMA((11,)),
            pltpu.SemaphoreType.DMA((len(NAMES),)),
            pltpu.SemaphoreType.DMA((len(NAMES),)),
            pltpu.SemaphoreType.DMA((8, 3)),
            pltpu.SemaphoreType.DMA((8, 3)),
            pltpu.SemaphoreType.DMA((8,)),
        ],
        compiler_params=pltpu.CompilerParams(
            collective_id=0, has_side_effects=True, vmem_limit_bytes=60 * 2**20
        ),
    )(slash, vert, place, which, q, k, v)


def shards(queries, keys, values, vertical, slash):
    slab = lax.axis_index("seq")
    ids = jnp.arange(256, dtype=jnp.int32)
    flat = vertical.reshape(-1)
    used = jnp.any(flat[:, None] == ids[None, :], axis=0)
    earlier = used[None, :] & (ids[None, :] // 8 == flat[:, None] // 8) & (ids[None, :] < flat[:, None])
    rank = jnp.sum(earlier.astype(jnp.int32), axis=1)
    place = jnp.concatenate([vertical // 8, 2 * rank.reshape(8, 8)], axis=0)
    mine = flat[:, None] - slab * 8
    slots = jnp.arange(4, dtype=jnp.int32)[None, :]
    hit = (mine >= 0) & (mine < 8) & (rank[:, None] == slots)
    which = jnp.max(jnp.where(hit, mine, 0), axis=0, keepdims=True)
    return attention(
        slash, vertical, place, which, queries, keys.reshape(8, BLK, BLK), values.reshape(8, BLK, BLK)
    )


def solution(mesh):
    return jax.shard_map(
        shards,
        mesh=mesh,
        in_specs=(P("seq", "head"), P("seq", "head"), P("seq", "head"), P("head", None), P("head", None)),
        out_specs=P(("seq", "head"), None),
        check_vma=False,
    )
```

```python
import functools, math
import jax, jax.numpy as jnp
from jax import lax
from jax.experimental import pallas as pl
from jax.experimental.pallas import tpu as pltpu
from jax.sharding import PartitionSpec as P

BLK = 128
NEG = -1e30
BACK = 28
F32 = jnp.float32
BF16 = jnp.bfloat16
SCALE2 = math.log2(math.e) / math.sqrt(128.0)


def dot(a, b):
    return jnp.dot(a, b, preferred_element_type=F32)


def lane_max(parts):
    top = parts[0]
    for part in parts[1:]:
        top = jnp.maximum(top, part)
    return jnp.max(top, axis=1, keepdims=True)


def lane_sum(parts):
    total = parts[0]
    for part in parts[1:]:
        total = total + part
    return jnp.sum(total, axis=1, keepdims=True)


def cat_dot(ps, vs):
    return dot(jnp.concatenate([p.astype(BF16) for p in ps], axis=1), jnp.concatenate(vs, axis=0))

def near_scores(h, i, slab, slash_ref, q_ref, ext_ref):
    rows = pl.ds(pl.multiple_of(i * BLK, BLK), BLK)
    q = q_ref[h, rows, :]
    row = lax.broadcasted_iota(jnp.int32, (BLK, BLK), 0)
    col = lax.broadcasted_iota(jnp.int32, (BLK, BLK), 1)
    own = BACK + i
    blocks = [own]
    bias = []
    for k in range(8):
        off = slash_ref[h, k]
        ok = slab * 8 + i - off >= 0
        blocks.append(jnp.where(ok, own - off, own))
        bias.append(jnp.where(ok, 0.0, NEG).astype(F32))
    scores = [jnp.where(row >= col, dot(q, ext_ref[own, 0]), NEG)]
    for k in range(0, 8, 2):
        both = dot(q, jnp.concatenate([ext_ref[blocks[1 + k], 0], ext_ref[blocks[2 + k], 0]], axis=1))
        scores.append(both[:, :BLK] + bias[k])
        scores.append(both[:, BLK:] + bias[k + 1])
    return scores, blocks, rows

def far_scores(h, i, slab, slash_ref, vert_ref, pos_ref, q_ref, far_ref):
    rows = pl.ds(pl.multiple_of(i * BLK, BLK), BLK)
    q = q_ref[h, rows, :]
    mine = slab * 8 + i
    bias, places = [], []
    for k in range(8):
        gap = mine - vert_ref[h, k]
        ok = gap > 0
        for n in range(8):
            ok = ok & (slash_ref[h, n] != gap)
        bias.append(jnp.where(ok, 0.0, NEG).astype(F32))
        places.append((jnp.where(ok, pos_ref[h, k], slab), jnp.where(ok, pos_ref[8 + h, k], 0)))
    scores = []
    for k in range(0, 8, 2):
        both = dot(q, jnp.concatenate([far_ref[places[k][0], places[k][1]], far_ref[places[k + 1][0], places[k + 1][1]]], axis=1))
        scores.append(both[:, :BLK] + bias[k])
        scores.append(both[:, BLK:] + bias[k + 1])
    return scores, places, rows

def near_put(slot, e, slab, slash, q, ext, stage):
    scores, _, _ = near_scores(e // 8, e % 8, slab, slash, q, ext)
    for k, s in enumerate(scores):
        stage[slot, k] = s


def near_finish(slot, e, slab, slash, ext, acc, top, tot, stage):
    h, i = e // 8, e % 8
    rows = pl.ds(pl.multiple_of(i * BLK, BLK), BLK)
    own = BACK + i
    blocks = [own]
    for k in range(8):
        off = slash[h, k]
        blocks.append(jnp.where(slab * 8 + i - off >= 0, own - off, own))
    scores = [stage[slot, k] for k in range(9)]
    best = lane_max(scores)
    weights = [jnp.exp2((s - best) * SCALE2) for s in scores]
    acc[h, rows, :] = cat_dot(weights, [ext[b, 1] for b in blocks])
    top[h, rows, :] = best
    tot[h, rows, :] = lane_sum(weights)


def far_put(slot, e, slab, slash, vert, pos, q, far, stage, spots):
    scores, places, _ = far_scores(e // 8, e % 8, slab, slash, vert, pos, q, far)
    for k, s in enumerate(scores):
        stage[slot, k] = s
        spots[slot, k] = places[k][0]
        spots[slot, 8 + k] = places[k][1]


def far_finish(slot, e, far, acc, top, tot, out, stage, spots):
    h, i = e // 8, e % 8
    rows = pl.ds(pl.multiple_of(i * BLK, BLK), BLK)
    scores = [stage[slot, k] for k in range(8)]
    old = top[h, rows, :]
    best = jnp.maximum(old, lane_max(scores))
    keep = jnp.exp2((old - best) * SCALE2)
    weights = [jnp.exp2((s - best) * SCALE2) for s in scores]
    mixed = cat_dot(weights, [far[spots[slot, k], spots[slot, 8 + k] + 1] for k in range(8)])
    total = tot[h, rows, :] * keep + lane_sum(weights)
    out[h, rows, :] = ((acc[h, rows, :] * keep + mixed) / total).astype(BF16)


MESH = pl.DeviceIdType.MESH
NEAR_STEPS = 4
FAR_STEPS = 4
DIRS = (1, -1)
NAMES = ["y", "zP2", "hA", "hB", "h3", "h4", "y1", "y2", "y3", "ro", "rp"]
NAMES += [kind + str(d) for kind in ("xo", "xp", "x1", "x2", "x3") for d in DIRS]
NAMES += [kind + n for kind in ("r", "s", "yr", "yq") for n in "123"]
NAMES += ["R" + str(j) + str(d) for j in (1, 2, 3) for d in DIRS]
NAMES += ["RR" + str(j) for j in (0, 1, 2, 3)]
NAMES += [kind + str(d) + n for kind in ("zP", "R0") for d in DIRS for n in "op"]
UPWARD = (2,)
BEFORE = (
    "+y", "+hA", "+hB", "+xo-1", "+zP-1o", "+R0-1o", "+xo1", "-y",
    "+xp-1", "+zP-1p", "+zP1o", "+zP1p", "-hA", "+y1", "+R0-1p", "-xo-1",
    "+ro", "-hB", "+h4", "-xp-1", "+rp", "-zP-1o", "-zP-1p", "+zP2",
    "-y1", "+h3", "+y2", "+x1-1", "-xo1", "+R11", "+x11", "+R3-1",
    "-zP2", "+x2-1", "+x21", "+R01p", "-h4", "+y3", "-zP1o", "-zP1p",
    "+x3-1", "-ro", "-rp", "+R21", "+R1-1", "-R1-1", "+RR1", "+yq1",
    "+x31", "-R0-1o", "-R0-1p", "+RR0", "-x1-1", "+r1", "-h3", "-y2",
    "-y3",
)
DURING = {
    1: ("-x2-1", "+r2",),
    2: ("+R01o",),
    3: ("+s2", "-RR1", "+yq2", "+xp1", "-R11", "+yq3",),
    6: ("+R31", "-R3-1", "+RR3",),
    7: ("+R2-1", "-x3-1", "+r3",),
    8: ("-R21", "+RR2", "+s1",),
    9: ("-r1", "+yr1",),
    11: ("-r2", "+yr2", "+s3",),
    12: ("-r3", "+yr3",),
}
AFTER = (
    "-R01o", "-R01p", "-xp1", "-x11", "-x21", "-x31", "-R31", "-R2-1",
    "-s1", "-yr1", "-yq1", "-s2", "-yr2", "-yq2", "-s3", "-yr3",
    "-yq3", "-RR0", "-RR2", "-RR3",
)
INDEX = {name: n for n, name in enumerate(NAMES)}


def kernel(slash, vert, place, which, q_hbm, k_hbm, v_hbm, out_hbm,
           q, raw, own, ext, far, acc, top, tot, out, stage, spots, load_sem, send_sem, recv_sem, part_sem, part_recv, keep_sem):
    group = lax.axis_index("head")
    slab = lax.axis_index("seq")
    x, z, half = slab // 8, (slab // 2) % 4, slab % 2
    loads = [
        pltpu.make_async_copy(k_hbm, raw, load_sem.at[8]),
        pltpu.make_async_copy(v_hbm, own.at[:, 1], load_sem.at[9]),
        pltpu.make_async_copy(v_hbm, ext.at[pl.ds(BACK, 8), 1], load_sem.at[10]),
    ]
    heads = [
        pltpu.make_async_copy(q_hbm.at[:, pl.ds(h * BLK, BLK)], q.at[h], load_sem.at[h]) for h in range(8)
    ]
    for load in loads + heads:
        load.start()

    def seat(dx, dz, dy):
        return ((x + dx) % 4) * 8 + ((z + dz) % 4) * 2 + ((half + dy) % 2)

    def spot(g, s):
        return (g, s)

    mate = spot(group, seat(0, 0, 1))
    after = spot(group, (slab + 2) % 32)
    before = spot(group, (slab + 30) % 32)
    across = {d: spot(group, seat(d, 0, 0)) for d in DIRS}
    along = {d: spot(group, seat(0, d, 0)) for d in DIRS}
    peers = [spot((group + n) % 4, slab) for n in (1, 2, 3)]
    barrier = pltpu.get_barrier_semaphore()
    friends = [mate, after, before, across[1], across[-1], along[1], along[-1]] + peers
    for friend in friends:
        pl.semaphore_signal(barrier, inc=1, device_id=friend, device_id_type=MESH)

    for load in loads:
        load.wait()
    for b in range(8):
        flipped = raw[b].astype(F32).T.astype(BF16)
        own[b, 0] = flipped
        ext[BACK + b, 0] = flipped
    for c in range(4):
        far[slab, 2 * c] = own[which[0, c], 0]
        far[slab, 2 * c + 1] = own[which[0, c], 1]
    pl.semaphore_wait(barrier, len(friends))

    PP, RR, ALL = (0, 4), (4, 4), (0, 8)

    def one(dx, dz, side, sub):
        return far.at[pl.ds(((x + dx) % 4) * 8 + ((z + dz) % 4) * 2 + side, 1), pl.ds(*sub)]

    def pair(dx, dz, sub):
        return far.at[pl.ds(((x + dx) % 4) * 8 + ((z + dz) % 4) * 2, 2), pl.ds(*sub)]

    def near(at, side_step=0):
        return ext.at[pl.ds(at + side_step * half, 4)]

    plan = {
        "y": (one(0, 0, half, ALL), None, mate, one(0, 0, 1 - half, ALL)),
        "zP2": (pair(0, 1, PP), None, along[-1], pair(0, 2, PP)),
        "hA": (near(28), near(12), after, near(12)),
        "hB": (near(32), near(16), after, near(16)),
        "h4": (near(16), near(0), after, near(0)),
        "h3": (near(20), near(4), after, near(4)),
        "y1": (near(28, -16), near(20), mate, near(20)),
        "y2": (near(32, -16), near(24), mate, near(24)),
        "y3": (near(16, -16), near(8), mate, near(8)),
    }
    sends = {d: x < 3 if d == 1 else x < 2 for d in DIRS}
    takes = {d: x > 0 if d == 1 else (x == 3) | (x == 0) for d in DIRS}
    sender, taker = {}, {}
    for d in DIRS:
        for n, source, lands in (
            ("xo", one(0, 0, half, ALL), one(-d, 0, half, ALL)),
            ("xp", one(0, 0, 1 - half, ALL), one(-d, 0, 1 - half, ALL)),
            ("x1", pair(0, 1, PP), pair(-d, 1, PP)),
            ("x2", pair(0, 2, PP), pair(-d, 2, PP)),
            ("x3", pair(0, -1, PP), pair(-d, -1, PP)),
        ):
            plan[n + str(d)] = (source, None, across[d], lands)
            sender[n + str(d)] = sends[d]
            taker[n + str(d)] = takes[d]
        for n, side in (("o", half), ("p", 1 - half)):
            plan["zP" + str(d) + n] = (one(0, 0, side, PP), None, along[d], one(0, -d, side, PP))
            plan["R0" + str(d) + n] = (one(0, 0, side, RR), None, along[d], one(0, -d, side, RR))
        for j in (1, 2, 3):
            part = (lambda dz: one(-1, dz, half, RR)) if j == 1 else (lambda dz, j=j: pair(-j, dz, RR))
            plan["R" + str(j) + str(d)] = (part(0), None, along[d], part(-d))
            sender["R" + str(j) + str(d)] = taker["R" + str(j) + str(d)] = x >= j
    for n, source, lands in (
        ("ro", one(1, 0, half, ALL), one(2, 0, half, ALL)),
        ("rp", one(1, 0, 1 - half, ALL), one(2, 0, 1 - half, ALL)),
        ("r1", one(1, 1, half, PP), one(2, 1, half, PP)),
        ("r2", one(1, 2, half, PP), one(2, 2, half, PP)),
        ("r3", one(1, -1, half, PP), one(2, -1, half, PP)),
    ):
        plan[n] = (source, None, across[-1], lands)
        sender[n] = (x == 0) | (x == 3)
        taker[n] = (x == 3) | (x == 2)
    for n, dz in (("1", 1), ("2", 2), ("3", -1)):
        plan["s" + n] = (one(1, dz, 1 - half, PP), None, across[-1], one(2, dz, 1 - half, PP))
        sender["s" + n] = x == 3
        taker["s" + n] = x == 2
        plan["yr" + n] = (one(2, dz, half, PP), None, mate, one(2, dz, 1 - half, PP))
        sender["yr" + n] = taker["yr" + n] = x == 3
        plan["yq" + n] = (one(-1, dz, half, RR), None, mate, one(-1, dz, 1 - half, RR))
        sender["yq" + n] = taker["yq" + n] = x >= 1
    for j in (0, 1, 2, 3):
        d = 1 if j in UPWARD else -1
        part = (lambda dz: one(-1, dz, half, RR)) if j == 1 else (lambda dz, j=j: pair(-j, dz, RR))
        plan["RR" + str(j)] = (part(-d), None, along[d], part(2))
        if j:
            sender["RR" + str(j)] = taker["RR" + str(j)] = x >= j

    def copy(name, landing):
        source, target, device, lands = plan[name]
        n = INDEX[name]
        return pltpu.make_async_remote_copy(
            src_ref=lands if landing else source,
            dst_ref=lands if landing else (source if target is None else target),
            send_sem=send_sem.at[n],
            recv_sem=recv_sem.at[n],
            device_id=device,
            device_id_type=MESH,
        )

    def guarded(rule, name, act):
        if name in rule:
            pl.when(rule[name])(act)
        else:
            act()

    def send(*names):
        for name in names:
            guarded(sender, name, lambda name=name: copy(name, False).start())

    waited = []

    def take(*names):
        for name in names:
            guarded(taker, name, lambda name=name: copy(name, True).wait_recv())
            waited.append(name)

    def run(steps):
        for step in steps:
            (take if step[0] == "-" else send)(step[1:])

    run(BEFORE)
    for head in heads:
        head.wait()

    near_put(0, 0, slab, slash, q, ext, stage)

    @pl.loop(0, 64 // NEAR_STEPS)
    def _(t):
        for when, steps in DURING.items():
            pl.when(t == when)(functools.partial(run, steps))
        for u in range(NEAR_STEPS):
            e = t * NEAR_STEPS + u
            near_put((u + 1) % 2, jnp.minimum(e + 1, 63), slab, slash, q, ext, stage)
            near_finish(u % 2, e, slab, slash, ext, acc, top, tot, stage)

    run(AFTER)
    take(*[name for name in NAMES if name not in waited])

    def quarter(h, n):
        return out.at[h, pl.ds(((group + n) % 4) * 256, 256)]

    def column(h):
        return out_hbm.at[:, pl.ds(pl.multiple_of((group * 8 + h) * BLK, BLK), BLK)]

    def share(h, n):
        return pltpu.make_async_remote_copy(
            src_ref=quarter(h, n),
            dst_ref=column(h),
            send_sem=part_sem.at[h, n - 1],
            recv_sem=part_recv.at[h, n - 1],
            device_id=peers[n - 1],
            device_id_type=MESH,
        )

    def keep(h):
        return pltpu.make_async_copy(quarter(h, 0), column(h), keep_sem.at[h])

    far_put(0, 0, slab, slash, vert, place, q, far, stage, spots)

    @pl.loop(0, 8)
    def _(h):
        @pl.loop(0, 8 // FAR_STEPS)
        def _(t):
            for u in range(FAR_STEPS):
                e = h * 8 + t * FAR_STEPS + u
                far_put((u + 1) % 2, jnp.minimum(e + 1, 63), slab, slash, vert, place, q, far, stage, spots)
                far_finish(u % 2, e, far, acc, top, tot, out, stage, spots)

        for n in (2, 1, 3):
            share(h, n).start()
        keep(h).start()

    for name in NAMES:
        guarded(sender, name, lambda name=name: copy(name, False).wait_send())

    @pl.loop(0, 8)
    def _(h):
        keep(h).wait()
        for n in (1, 2, 3):
            origin = (group - n + 4) % 4
            share(h, n).wait_send()
            lands = out_hbm.at[:, pl.ds(pl.multiple_of((origin * 8 + h) * BLK, BLK), BLK)]
            pltpu.make_async_remote_copy(
                src_ref=quarter(h, n),
                dst_ref=lands,
                send_sem=part_sem.at[h, n - 1],
                recv_sem=part_recv.at[h, n - 1],
                device_id=peers[n - 1],
                device_id_type=MESH,
            ).wait_recv()


def attention(slash, vert, place, which, q, k, v):
    whole = pl.BlockSpec(memory_space=pl.ANY)
    scalars = pl.BlockSpec(memory_space=pltpu.SMEM)
    return pl.pallas_call(
        kernel,
        out_shape=jax.ShapeDtypeStruct((256, 4096), BF16),
        in_specs=[scalars] * 4 + [whole] * 3,
        out_specs=whole,
        scratch_shapes=[
            pltpu.VMEM((8, 1024, 128), BF16),
            pltpu.VMEM((8, 128, 128), BF16),
            pltpu.VMEM((8, 2, 128, 128), BF16),
            pltpu.VMEM((36, 2, 128, 128), BF16),
            pltpu.VMEM((32, 8, 128, 128), BF16),
            pltpu.VMEM((8, 1024, 128), F32),
            pltpu.VMEM((8, 1024, 1), F32),
            pltpu.VMEM((8, 1024, 1), F32),
            pltpu.VMEM((8, 1024, 128), BF16),
            pltpu.VMEM((2, 9, 128, 128), F32),
            pltpu.SMEM((2, 16), jnp.int32),
            pltpu.SemaphoreType.DMA((11,)),
            pltpu.SemaphoreType.DMA((len(NAMES),)),
            pltpu.SemaphoreType.DMA((len(NAMES),)),
            pltpu.SemaphoreType.DMA((8, 3)),
            pltpu.SemaphoreType.DMA((8, 3)),
            pltpu.SemaphoreType.DMA((8,)),
        ],
        compiler_params=pltpu.CompilerParams(
            collective_id=0, has_side_effects=True, vmem_limit_bytes=60 * 2**20
        ),
    )(slash, vert, place, which, q, k, v)


def shards(queries, keys, values, vertical, slash):
    slab = lax.axis_index("seq")
    ids = jnp.arange(256, dtype=jnp.int32)
    flat = vertical.reshape(-1)
    used = jnp.any(flat[:, None] == ids[None, :], axis=0)
    earlier = used[None, :] & (ids[None, :] // 8 == flat[:, None] // 8) & (ids[None, :] < flat[:, None])
    rank = jnp.sum(earlier.astype(jnp.int32), axis=1)
    place = jnp.concatenate([vertical // 8, 2 * rank.reshape(8, 8)], axis=0)
    mine = flat[:, None] - slab * 8
    slots = jnp.arange(4, dtype=jnp.int32)[None, :]
    hit = (mine >= 0) & (mine < 8) & (rank[:, None] == slots)
    which = jnp.max(jnp.where(hit, mine, 0), axis=0, keepdims=True)
    return attention(
        slash, vertical, place, which, queries, keys.reshape(8, BLK, BLK), values.reshape(8, BLK, BLK)
    )


def solution(mesh):
    return jax.shard_map(
        shards,
        mesh=mesh,
        in_specs=(P("seq", "head"), P("seq", "head"), P("seq", "head"), P("head", None), P("head", None)),
        out_specs=P(("seq", "head"), None),
        check_vma=False,
    )
```

```python
import functools, math
import jax, jax.numpy as jnp
from jax import lax
from jax.experimental import pallas as pl
from jax.experimental.pallas import tpu as pltpu
from jax.sharding import PartitionSpec as P

BLK = 128
NEG = -1e30
BACK = 28
F32 = jnp.float32
BF16 = jnp.bfloat16
SCALE2 = math.log2(math.e) / math.sqrt(128.0)


def dot(a, b):
    return jnp.dot(a, b, preferred_element_type=F32)


def lane_max(parts):
    top = parts[0]
    for part in parts[1:]:
        top = jnp.maximum(top, part)
    return jnp.max(top, axis=1, keepdims=True)


def lane_sum(parts):
    total = parts[0]
    for part in parts[1:]:
        total = total + part
    return jnp.sum(total, axis=1, keepdims=True)


def cat_dot(ps, vs):
    return dot(jnp.concatenate([p.astype(BF16) for p in ps], axis=1), jnp.concatenate(vs, axis=0))

def near_scores(h, i, slab, slash_ref, q_ref, ext_ref):
    rows = pl.ds(pl.multiple_of(i * BLK, BLK), BLK)
    q = q_ref[h, rows, :]
    row = lax.broadcasted_iota(jnp.int32, (BLK, BLK), 0)
    col = lax.broadcasted_iota(jnp.int32, (BLK, BLK), 1)
    own = BACK + i
    blocks = [own]
    bias = []
    for k in range(8):
        off = slash_ref[h, k]
        ok = slab * 8 + i - off >= 0
        blocks.append(jnp.where(ok, own - off, own))
        bias.append(jnp.where(ok, 0.0, NEG).astype(F32))
    scores = [jnp.where(row >= col, dot(q, ext_ref[own, 0]), NEG)]
    for k in range(0, 8, 2):
        both = dot(q, jnp.concatenate([ext_ref[blocks[1 + k], 0], ext_ref[blocks[2 + k], 0]], axis=1))
        scores.append(both[:, :BLK] + bias[k])
        scores.append(both[:, BLK:] + bias[k + 1])
    return scores, blocks, rows

def far_scores(h, i, slab, slash_ref, vert_ref, pos_ref, q_ref, far_ref):
    rows = pl.ds(pl.multiple_of(i * BLK, BLK), BLK)
    q = q_ref[h, rows, :]
    mine = slab * 8 + i
    bias, places = [], []
    for k in range(8):
        gap = mine - vert_ref[h, k]
        ok = gap > 0
        for n in range(8):
            ok = ok & (slash_ref[h, n] != gap)
        bias.append(jnp.where(ok, 0.0, NEG).astype(F32))
        places.append((jnp.where(ok, pos_ref[h, k], slab), jnp.where(ok, pos_ref[8 + h, k], 0)))
    scores = []
    for k in range(0, 8, 2):
        both = dot(q, jnp.concatenate([far_ref[places[k][0], places[k][1]], far_ref[places[k + 1][0], places[k + 1][1]]], axis=1))
        scores.append(both[:, :BLK] + bias[k])
        scores.append(both[:, BLK:] + bias[k + 1])
    return scores, places, rows

def near_put(slot, e, slab, slash, q, ext, stage):
    scores, _, _ = near_scores(e // 8, e % 8, slab, slash, q, ext)
    for k, s in enumerate(scores):
        stage[slot, k] = s


def near_finish(slot, e, slab, slash, ext, acc, top, tot, stage):
    h, i = e // 8, e % 8
    rows = pl.ds(pl.multiple_of(i * BLK, BLK), BLK)
    own = BACK + i
    blocks = [own]
    for k in range(8):
        off = slash[h, k]
        blocks.append(jnp.where(slab * 8 + i - off >= 0, own - off, own))
    scores = [stage[slot, k] for k in range(9)]
    best = lane_max(scores)
    weights = [jnp.exp2((s - best) * SCALE2) for s in scores]
    acc[h, rows, :] = cat_dot(weights, [ext[b, 1] for b in blocks])
    top[h, rows, :] = best
    tot[h, rows, :] = lane_sum(weights)


def far_put(slot, e, slab, slash, vert, pos, q, far, stage, spots):
    scores, places, _ = far_scores(e // 8, e % 8, slab, slash, vert, pos, q, far)
    for k, s in enumerate(scores):
        stage[slot, k] = s
        spots[slot, k] = places[k][0]
        spots[slot, 8 + k] = places[k][1]


def far_finish(slot, e, far, acc, top, tot, out, stage, spots):
    h, i = e // 8, e % 8
    rows = pl.ds(pl.multiple_of(i * BLK, BLK), BLK)
    scores = [stage[slot, k] for k in range(8)]
    old = top[h, rows, :]
    best = jnp.maximum(old, lane_max(scores))
    keep = jnp.exp2((old - best) * SCALE2)
    weights = [jnp.exp2((s - best) * SCALE2) for s in scores]
    mixed = cat_dot(weights, [far[spots[slot, k], spots[slot, 8 + k] + 1] for k in range(8)])
    total = tot[h, rows, :] * keep + lane_sum(weights)
    out[h, rows, :] = ((acc[h, rows, :] * keep + mixed) / total).astype(BF16)


MESH = pl.DeviceIdType.MESH
NEAR_STEPS = 4
FAR_STEPS = 4
DIRS = (1, -1)
NAMES = ["y", "zP2", "hA", "hB", "h3", "h4", "y1", "y2", "y3", "ro", "rp"]
NAMES += [kind + str(d) for kind in ("xo", "xp", "x1", "x2", "x3") for d in DIRS]
NAMES += [kind + n for kind in ("r", "s", "yr", "yq") for n in "123"]
NAMES += ["R" + str(j) + str(d) for j in (1, 2, 3) for d in DIRS]
NAMES += ["RR" + str(j) for j in (0, 1, 2, 3)]
NAMES += [kind + str(d) + n for kind in ("zP", "R0") for d in DIRS for n in "op"]
UPWARD = (2,)
BEFORE = (
    "+y", "+hA", "+hB", "+xo-1", "+zP-1o", "+R0-1o", "+xo1", "-y",
    "+xp-1", "+zP-1p", "+zP1o", "+zP1p", "-hA", "+y1", "+R0-1p", "-xo-1",
    "+ro", "-hB", "+h4", "-xp-1", "+rp", "-zP-1o", "-zP-1p", "+zP2",
    "-y1", "+h3", "+y2", "+x1-1", "-xo1", "+R11", "+x11", "+R3-1",
    "-zP2", "+x2-1", "+x21", "+R01p", "-h4", "+y3", "-zP1o", "-zP1p",
    "+x3-1", "-ro", "-rp", "+R21", "+R1-1", "-R1-1", "+RR1", "+yq1",
    "+x31", "-R0-1o", "-R0-1p", "+RR0", "-x1-1", "+r1", "-h3", "-y2",
    "-y3",
)
DURING = {
    1: ("-x2-1", "+r2",),
    2: ("+R01o",),
    3: ("+s2", "-RR1", "+yq2", "+xp1", "-R11", "+yq3",),
    6: ("+R31", "-R3-1", "+RR3",),
    7: ("+R2-1", "-x3-1", "+r3",),
    8: ("-R21", "+RR2", "+s1",),
    9: ("-r1", "+yr1",),
    11: ("-r2", "+yr2", "+s3",),
    12: ("-r3", "+yr3",),
}
AFTER = (
    "-R01o", "-R01p", "-xp1", "-x11", "-x21", "-x31", "-R31", "-R2-1",
    "-s1", "-yr1", "-yq1", "-s2", "-yr2", "-yq2", "-s3", "-yr3",
    "-yq3", "-RR0", "-RR2", "-RR3",
)
INDEX = {name: n for n, name in enumerate(NAMES)}


def kernel(slash, vert, place, which, q_hbm, k_hbm, v_hbm, out_hbm,
           q, raw, own, ext, far, acc, top, tot, out, stage, spots, load_sem, send_sem, recv_sem, part_sem, part_recv, keep_sem):
    group = lax.axis_index("head")
    slab = lax.axis_index("seq")
    x, z, half = slab // 8, (slab // 2) % 4, slab % 2
    loads = [
        pltpu.make_async_copy(k_hbm, raw, load_sem.at[8]),
        pltpu.make_async_copy(v_hbm, own.at[:, 1], load_sem.at[9]),
        pltpu.make_async_copy(v_hbm, ext.at[pl.ds(BACK, 8), 1], load_sem.at[10]),
    ]
    heads = [
        pltpu.make_async_copy(q_hbm.at[:, pl.ds(h * BLK, BLK)], q.at[h], load_sem.at[h]) for h in range(8)
    ]
    for load in loads + heads:
        load.start()

    def seat(dx, dz, dy):
        return ((x + dx) % 4) * 8 + ((z + dz) % 4) * 2 + ((half + dy) % 2)

    def spot(g, s):
        return (g, s)

    mate = spot(group, seat(0, 0, 1))
    after = spot(group, (slab + 2) % 32)
    before = spot(group, (slab + 30) % 32)
    across = {d: spot(group, seat(d, 0, 0)) for d in DIRS}
    along = {d: spot(group, seat(0, d, 0)) for d in DIRS}
    peers = [spot((group + n) % 4, slab) for n in (1, 2, 3)]
    barrier = pltpu.get_barrier_semaphore()
    friends = [mate, after, before, across[1], across[-1], along[1], along[-1]] + peers
    for friend in friends:
        pl.semaphore_signal(barrier, inc=1, device_id=friend, device_id_type=MESH)

    for load in loads:
        load.wait()
    for b in range(8):
        flipped = raw[b].astype(F32).T.astype(BF16)
        own[b, 0] = flipped
        ext[BACK + b, 0] = flipped
    for c in range(4):
        far[slab, 2 * c] = own[which[0, c], 0]
        far[slab, 2 * c + 1] = own[which[0, c], 1]
    pl.semaphore_wait(barrier, len(friends))

    PP, RR, ALL = (0, 4), (4, 4), (0, 8)

    def one(dx, dz, side, sub):
        return far.at[pl.ds(((x + dx) % 4) * 8 + ((z + dz) % 4) * 2 + side, 1), pl.ds(*sub)]

    def pair(dx, dz, sub):
        return far.at[pl.ds(((x + dx) % 4) * 8 + ((z + dz) % 4) * 2, 2), pl.ds(*sub)]

    def near(at, side_step=0):
        return ext.at[pl.ds(at + side_step * half, 4)]

    plan = {
        "y": (one(0, 0, half, ALL), None, mate, one(0, 0, 1 - half, ALL)),
        "zP2": (pair(0, 1, PP), None, along[-1], pair(0, 2, PP)),
        "hA": (near(28), near(12), after, near(12)),
        "hB": (near(32), near(16), after, near(16)),
        "h4": (near(16), near(0), after, near(0)),
        "h3": (near(20), near(4), after, near(4)),
        "y1": (near(28, -16), near(20), mate, near(20)),
        "y2": (near(32, -16), near(24), mate, near(24)),
        "y3": (near(16, -16), near(8), mate, near(8)),
    }
    sends = {d: x < 3 if d == 1 else x < 2 for d in DIRS}
    takes = {d: x > 0 if d == 1 else (x == 3) | (x == 0) for d in DIRS}
    sender, taker = {}, {}
    for d in DIRS:
        for n, source, lands in (
            ("xo", one(0, 0, half, ALL), one(-d, 0, half, ALL)),
            ("xp", one(0, 0, 1 - half, ALL), one(-d, 0, 1 - half, ALL)),
            ("x1", pair(0, 1, PP), pair(-d, 1, PP)),
            ("x2", pair(0, 2, PP), pair(-d, 2, PP)),
            ("x3", pair(0, -1, PP), pair(-d, -1, PP)),
        ):
            plan[n + str(d)] = (source, None, across[d], lands)
            sender[n + str(d)] = sends[d]
            taker[n + str(d)] = takes[d]
        for n, side in (("o", half), ("p", 1 - half)):
            plan["zP" + str(d) + n] = (one(0, 0, side, PP), None, along[d], one(0, -d, side, PP))
            plan["R0" + str(d) + n] = (one(0, 0, side, RR), None, along[d], one(0, -d, side, RR))
        for j in (1, 2, 3):
            part = (lambda dz: one(-1, dz, half, RR)) if j == 1 else (lambda dz, j=j: pair(-j, dz, RR))
            plan["R" + str(j) + str(d)] = (part(0), None, along[d], part(-d))
            sender["R" + str(j) + str(d)] = taker["R" + str(j) + str(d)] = x >= j
    for n, source, lands in (
        ("ro", one(1, 0, half, ALL), one(2, 0, half, ALL)),
        ("rp", one(1, 0, 1 - half, ALL), one(2, 0, 1 - half, ALL)),
        ("r1", one(1, 1, half, PP), one(2, 1, half, PP)),
        ("r2", one(1, 2, half, PP), one(2, 2, half, PP)),
        ("r3", one(1, -1, half, PP), one(2, -1, half, PP)),
    ):
        plan[n] = (source, None, across[-1], lands)
        sender[n] = (x == 0) | (x == 3)
        taker[n] = (x == 3) | (x == 2)
    for n, dz in (("1", 1), ("2", 2), ("3", -1)):
        plan["s" + n] = (one(1, dz, 1 - half, PP), None, across[-1], one(2, dz, 1 - half, PP))
        sender["s" + n] = x == 3
        taker["s" + n] = x == 2
        plan["yr" + n] = (one(2, dz, half, PP), None, mate, one(2, dz, 1 - half, PP))
        sender["yr" + n] = taker["yr" + n] = x == 3
        plan["yq" + n] = (one(-1, dz, half, RR), None, mate, one(-1, dz, 1 - half, RR))
        sender["yq" + n] = taker["yq" + n] = x >= 1
    for j in (0, 1, 2, 3):
        d = 1 if j in UPWARD else -1
        part = (lambda dz: one(-1, dz, half, RR)) if j == 1 else (lambda dz, j=j: pair(-j, dz, RR))
        plan["RR" + str(j)] = (part(-d), None, along[d], part(2))
        if j:
            sender["RR" + str(j)] = taker["RR" + str(j)] = x >= j

    def copy(name, landing):
        source, target, device, lands = plan[name]
        n = INDEX[name]
        return pltpu.make_async_remote_copy(
            src_ref=lands if landing else source,
            dst_ref=lands if landing else (source if target is None else target),
            send_sem=send_sem.at[n],
            recv_sem=recv_sem.at[n],
            device_id=device,
            device_id_type=MESH,
        )

    def guarded(rule, name, act):
        if name in rule:
            pl.when(rule[name])(act)
        else:
            act()

    def send(*names):
        for name in names:
            guarded(sender, name, lambda name=name: copy(name, False).start())

    waited = []

    def take(*names):
        for name in names:
            guarded(taker, name, lambda name=name: copy(name, True).wait_recv())
            waited.append(name)

    def run(steps):
        for step in steps:
            (take if step[0] == "-" else send)(step[1:])

    run(BEFORE)
    for head in heads:
        head.wait()

    near_put(0, 0, slab, slash, q, ext, stage)

    @pl.loop(0, 64 // NEAR_STEPS)
    def _(t):
        for when, steps in DURING.items():
            pl.when(t == when)(functools.partial(run, steps))
        for u in range(NEAR_STEPS):
            e = t * NEAR_STEPS + u
            near_put((u + 1) % 2, jnp.minimum(e + 1, 63), slab, slash, q, ext, stage)
            near_finish(u % 2, e, slab, slash, ext, acc, top, tot, stage)

    run(AFTER)
    take(*[name for name in NAMES if name not in waited])

    def quarter(h, n):
        return out.at[h, pl.ds(((group + n) % 4) * 256, 256)]

    def column(h):
        return out_hbm.at[:, pl.ds(pl.multiple_of((group * 8 + h) * BLK, BLK), BLK)]

    def share(h, n):
        return pltpu.make_async_remote_copy(
            src_ref=quarter(h, n),
            dst_ref=column(h),
            send_sem=part_sem.at[h, n - 1],
            recv_sem=part_recv.at[h, n - 1],
            device_id=peers[n - 1],
            device_id_type=MESH,
        )

    def keep(h):
        return pltpu.make_async_copy(quarter(h, 0), column(h), keep_sem.at[h])

    far_put(0, 0, slab, slash, vert, place, q, far, stage, spots)

    @pl.loop(0, 8)
    def _(h):
        @pl.loop(0, 8 // FAR_STEPS)
        def _(t):
            for u in range(FAR_STEPS):
                e = h * 8 + t * FAR_STEPS + u
                far_put((u + 1) % 2, jnp.minimum(e + 1, 63), slab, slash, vert, place, q, far, stage, spots)
                far_finish(u % 2, e, far, acc, top, tot, out, stage, spots)
            for n in (2, 1, 3):
                pl.when(((group + n) % 4) // 2 == t)(lambda n=n: share(h, n).start())
            pl.when(group // 2 == t)(lambda: keep(h).start())


    for name in NAMES:
        guarded(sender, name, lambda name=name: copy(name, False).wait_send())

    @pl.loop(0, 8)
    def _(h):
        keep(h).wait()
        for n in (1, 2, 3):
            origin = (group - n + 4) % 4
            share(h, n).wait_send()
            lands = out_hbm.at[:, pl.ds(pl.multiple_of((origin * 8 + h) * BLK, BLK), BLK)]
            pltpu.make_async_remote_copy(
                src_ref=quarter(h, n),
                dst_ref=lands,
                send_sem=part_sem.at[h, n - 1],
                recv_sem=part_recv.at[h, n - 1],
                device_id=peers[n - 1],
                device_id_type=MESH,
            ).wait_recv()


def attention(slash, vert, place, which, q, k, v):
    whole = pl.BlockSpec(memory_space=pl.ANY)
    scalars = pl.BlockSpec(memory_space=pltpu.SMEM)
    return pl.pallas_call(
        kernel,
        out_shape=jax.ShapeDtypeStruct((256, 4096), BF16),
        in_specs=[scalars] * 4 + [whole] * 3,
        out_specs=whole,
        scratch_shapes=[
            pltpu.VMEM((8, 1024, 128), BF16),
            pltpu.VMEM((8, 128, 128), BF16),
            pltpu.VMEM((8, 2, 128, 128), BF16),
            pltpu.VMEM((36, 2, 128, 128), BF16),
            pltpu.VMEM((32, 8, 128, 128), BF16),
            pltpu.VMEM((8, 1024, 128), F32),
            pltpu.VMEM((8, 1024, 1), F32),
            pltpu.VMEM((8, 1024, 1), F32),
            pltpu.VMEM((8, 1024, 128), BF16),
            pltpu.VMEM((2, 9, 128, 128), F32),
            pltpu.SMEM((2, 16), jnp.int32),
            pltpu.SemaphoreType.DMA((11,)),
            pltpu.SemaphoreType.DMA((len(NAMES),)),
            pltpu.SemaphoreType.DMA((len(NAMES),)),
            pltpu.SemaphoreType.DMA((8, 3)),
            pltpu.SemaphoreType.DMA((8, 3)),
            pltpu.SemaphoreType.DMA((8,)),
        ],
        compiler_params=pltpu.CompilerParams(
            collective_id=0, has_side_effects=True, vmem_limit_bytes=60 * 2**20
        ),
    )(slash, vert, place, which, q, k, v)


def shards(queries, keys, values, vertical, slash):
    slab = lax.axis_index("seq")
    ids = jnp.arange(256, dtype=jnp.int32)
    flat = vertical.reshape(-1)
    used = jnp.any(flat[:, None] == ids[None, :], axis=0)
    earlier = used[None, :] & (ids[None, :] // 8 == flat[:, None] // 8) & (ids[None, :] < flat[:, None])
    rank = jnp.sum(earlier.astype(jnp.int32), axis=1)
    place = jnp.concatenate([vertical // 8, 2 * rank.reshape(8, 8)], axis=0)
    mine = flat[:, None] - slab * 8
    slots = jnp.arange(4, dtype=jnp.int32)[None, :]
    hit = (mine >= 0) & (mine < 8) & (rank[:, None] == slots)
    which = jnp.max(jnp.where(hit, mine, 0), axis=0, keepdims=True)
    return attention(
        slash, vertical, place, which, queries, keys.reshape(8, BLK, BLK), values.reshape(8, BLK, BLK)
    )


def solution(mesh):
    return jax.shard_map(
        shards,
        mesh=mesh,
        in_specs=(P("seq", "head"), P("seq", "head"), P("seq", "head"), P("head", None), P("head", None)),
        out_specs=P(("seq", "head"), None),
        check_vma=False,
    )
```

```python
import functools, math
import jax, jax.numpy as jnp
from jax import lax
from jax.experimental import pallas as pl
from jax.experimental.pallas import tpu as pltpu
from jax.sharding import PartitionSpec as P

BLK = 128
NEG = -1e30
BACK = 28
F32 = jnp.float32
BF16 = jnp.bfloat16
SCALE2 = math.log2(math.e) / math.sqrt(128.0)


def dot(a, b):
    return jnp.dot(a, b, preferred_element_type=F32)


def lane_max(parts):
    top = parts[0]
    for part in parts[1:]:
        top = jnp.maximum(top, part)
    return jnp.max(top, axis=1, keepdims=True)


def lane_sum(parts):
    total = parts[0]
    for part in parts[1:]:
        total = total + part
    return jnp.sum(total, axis=1, keepdims=True)


def cat_dot(ps, vs):
    return dot(jnp.concatenate([p.astype(BF16) for p in ps], axis=1), jnp.concatenate(vs, axis=0))

def near_scores(h, i, slab, slash_ref, q_ref, ext_ref):
    rows = pl.ds(pl.multiple_of(i * BLK, BLK), BLK)
    q = q_ref[h, rows, :]
    row = lax.broadcasted_iota(jnp.int32, (BLK, BLK), 0)
    col = lax.broadcasted_iota(jnp.int32, (BLK, BLK), 1)
    own = BACK + i
    blocks = [own]
    bias = []
    for k in range(8):
        off = slash_ref[h, k]
        ok = slab * 8 + i - off >= 0
        blocks.append(jnp.where(ok, own - off, own))
        bias.append(jnp.where(ok, 0.0, NEG).astype(F32))
    scores = [jnp.where(row >= col, dot(q, ext_ref[own, 0]), NEG)]
    for k in range(0, 8, 2):
        both = dot(q, jnp.concatenate([ext_ref[blocks[1 + k], 0], ext_ref[blocks[2 + k], 0]], axis=1))
        scores.append(both[:, :BLK] + bias[k])
        scores.append(both[:, BLK:] + bias[k + 1])
    return scores, blocks, rows

def far_scores(h, i, slab, slash_ref, vert_ref, pos_ref, q_ref, far_ref):
    rows = pl.ds(pl.multiple_of(i * BLK, BLK), BLK)
    q = q_ref[h, rows, :]
    mine = slab * 8 + i
    bias, places = [], []
    for k in range(8):
        gap = mine - vert_ref[h, k]
        ok = gap > 0
        for n in range(8):
            ok = ok & (slash_ref[h, n] != gap)
        bias.append(jnp.where(ok, 0.0, NEG).astype(F32))
        places.append((jnp.where(ok, pos_ref[h, k], slab), jnp.where(ok, pos_ref[8 + h, k], 0)))
    scores = []
    for k in range(0, 8, 2):
        both = dot(q, jnp.concatenate([far_ref[places[k][0], places[k][1]], far_ref[places[k + 1][0], places[k + 1][1]]], axis=1))
        scores.append(both[:, :BLK] + bias[k])
        scores.append(both[:, BLK:] + bias[k + 1])
    return scores, places, rows

def near_put(slot, e, slab, slash, q, ext, stage):
    scores, _, _ = near_scores(e // 8, e % 8, slab, slash, q, ext)
    for k, s in enumerate(scores):
        stage[slot, k] = s


def near_finish(slot, e, slab, slash, ext, acc, top, tot, stage):
    h, i = e // 8, e % 8
    rows = pl.ds(pl.multiple_of(i * BLK, BLK), BLK)
    own = BACK + i
    blocks = [own]
    for k in range(8):
        off = slash[h, k]
        blocks.append(jnp.where(slab * 8 + i - off >= 0, own - off, own))
    scores = [stage[slot, k] for k in range(9)]
    best = lane_max(scores)
    weights = [jnp.exp2((s - best) * SCALE2) for s in scores]
    acc[h, rows, :] = cat_dot(weights, [ext[b, 1] for b in blocks])
    top[h, rows, :] = best
    tot[h, rows, :] = lane_sum(weights)


def far_put(slot, e, slab, slash, vert, pos, q, far, stage, spots):
    scores, places, _ = far_scores(e // 8, e % 8, slab, slash, vert, pos, q, far)
    for k, s in enumerate(scores):
        stage[slot, k] = s
        spots[slot, k] = places[k][0]
        spots[slot, 8 + k] = places[k][1]


def far_finish(slot, e, far, acc, top, tot, out, stage, spots):
    h, i = e // 8, e % 8
    rows = pl.ds(pl.multiple_of(i * BLK, BLK), BLK)
    scores = [stage[slot, k] for k in range(8)]
    old = top[h, rows, :]
    best = jnp.maximum(old, lane_max(scores))
    keep = jnp.exp2((old - best) * SCALE2)
    weights = [jnp.exp2((s - best) * SCALE2) for s in scores]
    mixed = cat_dot(weights, [far[spots[slot, k], spots[slot, 8 + k] + 1] for k in range(8)])
    total = tot[h, rows, :] * keep + lane_sum(weights)
    out[h, rows, :] = ((acc[h, rows, :] * keep + mixed) / total).astype(BF16)


MESH = pl.DeviceIdType.MESH
NEAR_STEPS = 4
FAR_STEPS = 4
DIRS = (1, -1)
NAMES = ["y", "zP2", "hA", "hB", "h3", "h4", "y1", "y2", "y3", "ro", "rp"]
NAMES += [kind + str(d) for kind in ("xo", "xp", "x1", "x2", "x3") for d in DIRS]
NAMES += [kind + n for kind in ("r", "s", "yr", "yq") for n in "123"]
NAMES += ["R" + str(j) + str(d) for j in (1, 2, 3) for d in DIRS]
NAMES += ["RR" + str(j) for j in (0, 1, 2, 3)]
NAMES += [kind + str(d) + n for kind in ("zP", "R0") for d in DIRS for n in "op"]
UPWARD = (2,)
BEFORE = (
    "+y", "+hA", "+hB", "+xo-1", "+zP-1o", "+R0-1o", "+xo1", "-y",
    "+xp-1", "+zP-1p", "+zP1o", "+zP1p", "-hA", "+y1", "+R0-1p", "-xo-1",
    "+ro", "-hB", "+h4", "-xp-1", "+rp", "-zP-1o", "-zP-1p", "+zP2",
    "-y1", "+h3", "+y2", "+x1-1", "-xo1", "+R11", "+x11", "+R3-1",
    "-zP2", "+x2-1", "+x21", "+R01p", "-h4", "+y3", "-zP1o", "-zP1p",
    "+x3-1", "-ro", "-rp", "+R21", "+R1-1", "-R1-1", "+RR1", "+yq1",
    "+x31", "-R0-1o", "-R0-1p", "+RR0", "-x1-1", "+r1", "-h3", "-y2",
    "-y3",
)
DURING = {
    1: ("-x2-1", "+r2",),
    2: ("+R01o",),
    3: ("+s2", "-RR1", "+yq2", "+xp1", "-R11", "+yq3",),
    6: ("+R31", "-R3-1", "+RR3",),
    7: ("+R2-1", "-x3-1", "+r3",),
    8: ("-R21", "+RR2", "+s1",),
    9: ("-r1", "+yr1",),
    11: ("-r2", "+yr2", "+s3",),
    12: ("-r3", "+yr3",),
}
AFTER = (
    "-R01o", "-R01p", "-xp1", "-x11", "-x21", "-x31", "-R31", "-R2-1",
    "-s1", "-yr1", "-yq1", "-s2", "-yr2", "-yq2", "-s3", "-yr3",
    "-yq3", "-RR0", "-RR2", "-RR3",
)
INDEX = {name: n for n, name in enumerate(NAMES)}


def seen(vert, slab):
    mask = jnp.int32(0)
    for h in range(8):
        for k in range(8):
            name = vert[h, k]
            mask = mask | jnp.where((name >> 3) == slab, jnp.int32(1) << (name & 7), 0)
    return mask


def kernel(slash, vert, q_hbm, k_hbm, v_hbm, out_hbm,
           q, raw, own, ext, far, acc, top, tot, out, stage, spots, marks, place, load_sem, send_sem, recv_sem, part_sem, part_recv, keep_sem):
    group = lax.axis_index("head")
    slab = lax.axis_index("seq")
    x, z, half = slab // 8, (slab // 2) % 4, slab % 2
    loads = [
        pltpu.make_async_copy(k_hbm, raw, load_sem.at[8]),
        pltpu.make_async_copy(v_hbm, own.at[:, 1], load_sem.at[9]),
        pltpu.make_async_copy(v_hbm, ext.at[pl.ds(BACK, 8), 1], load_sem.at[10]),
    ]
    heads = [
        pltpu.make_async_copy(q_hbm.at[:, pl.ds(h * BLK, BLK)], q.at[h], load_sem.at[h]) for h in range(8)
    ]
    for load in loads + heads:
        load.start()

    def seat(dx, dz, dy):
        return ((x + dx) % 4) * 8 + ((z + dz) % 4) * 2 + ((half + dy) % 2)

    def spot(g, s):
        return (g, s)

    mate = spot(group, seat(0, 0, 1))
    after = spot(group, (slab + 2) % 32)
    before = spot(group, (slab + 30) % 32)
    across = {d: spot(group, seat(d, 0, 0)) for d in DIRS}
    along = {d: spot(group, seat(0, d, 0)) for d in DIRS}
    peers = [spot((group + n) % 4, slab) for n in (1, 2, 3)]
    barrier = pltpu.get_barrier_semaphore()
    friends = [mate, after, before, across[1], across[-1], along[1], along[-1]] + peers
    for friend in friends:
        pl.semaphore_signal(barrier, inc=1, device_id=friend, device_id_type=MESH)

    mask, count, chosen = seen(vert, slab), jnp.int32(0), [jnp.int32(0)] * 4
    for b in range(8):
        bit = (mask >> b) & 1
        for c in range(4):
            chosen[c] = jnp.where((bit == 1) & (count == c), b, chosen[c])
        count = count + bit

    for load in loads:
        load.wait()
    for b in range(8):
        flipped = raw[b].astype(F32).T.astype(BF16)
        own[b, 0] = flipped
        ext[BACK + b, 0] = flipped
    for c in range(4):
        far[slab, 2 * c] = own[chosen[c], 0]
        far[slab, 2 * c + 1] = own[chosen[c], 1]
    pl.semaphore_wait(barrier, len(friends))

    PP, RR, ALL = (0, 4), (4, 4), (0, 8)

    def one(dx, dz, side, sub):
        return far.at[pl.ds(((x + dx) % 4) * 8 + ((z + dz) % 4) * 2 + side, 1), pl.ds(*sub)]

    def pair(dx, dz, sub):
        return far.at[pl.ds(((x + dx) % 4) * 8 + ((z + dz) % 4) * 2, 2), pl.ds(*sub)]

    def near(at, side_step=0):
        return ext.at[pl.ds(at + side_step * half, 4)]

    plan = {
        "y": (one(0, 0, half, ALL), None, mate, one(0, 0, 1 - half, ALL)),
        "zP2": (pair(0, 1, PP), None, along[-1], pair(0, 2, PP)),
        "hA": (near(28), near(12), after, near(12)),
        "hB": (near(32), near(16), after, near(16)),
        "h4": (near(16), near(0), after, near(0)),
        "h3": (near(20), near(4), after, near(4)),
        "y1": (near(28, -16), near(20), mate, near(20)),
        "y2": (near(32, -16), near(24), mate, near(24)),
        "y3": (near(16, -16), near(8), mate, near(8)),
    }
    sends = {d: x < 3 if d == 1 else x < 2 for d in DIRS}
    takes = {d: x > 0 if d == 1 else (x == 3) | (x == 0) for d in DIRS}
    sender, taker = {}, {}
    for d in DIRS:
        for n, source, lands in (
            ("xo", one(0, 0, half, ALL), one(-d, 0, half, ALL)),
            ("xp", one(0, 0, 1 - half, ALL), one(-d, 0, 1 - half, ALL)),
            ("x1", pair(0, 1, PP), pair(-d, 1, PP)),
            ("x2", pair(0, 2, PP), pair(-d, 2, PP)),
            ("x3", pair(0, -1, PP), pair(-d, -1, PP)),
        ):
            plan[n + str(d)] = (source, None, across[d], lands)
            sender[n + str(d)] = sends[d]
            taker[n + str(d)] = takes[d]
        for n, side in (("o", half), ("p", 1 - half)):
            plan["zP" + str(d) + n] = (one(0, 0, side, PP), None, along[d], one(0, -d, side, PP))
            plan["R0" + str(d) + n] = (one(0, 0, side, RR), None, along[d], one(0, -d, side, RR))
        for j in (1, 2, 3):
            part = (lambda dz: one(-1, dz, half, RR)) if j == 1 else (lambda dz, j=j: pair(-j, dz, RR))
            plan["R" + str(j) + str(d)] = (part(0), None, along[d], part(-d))
            sender["R" + str(j) + str(d)] = taker["R" + str(j) + str(d)] = x >= j
    for n, source, lands in (
        ("ro", one(1, 0, half, ALL), one(2, 0, half, ALL)),
        ("rp", one(1, 0, 1 - half, ALL), one(2, 0, 1 - half, ALL)),
        ("r1", one(1, 1, half, PP), one(2, 1, half, PP)),
        ("r2", one(1, 2, half, PP), one(2, 2, half, PP)),
        ("r3", one(1, -1, half, PP), one(2, -1, half, PP)),
    ):
        plan[n] = (source, None, across[-1], lands)
        sender[n] = (x == 0) | (x == 3)
        taker[n] = (x == 3) | (x == 2)
    for n, dz in (("1", 1), ("2", 2), ("3", -1)):
        plan["s" + n] = (one(1, dz, 1 - half, PP), None, across[-1], one(2, dz, 1 - half, PP))
        sender["s" + n] = x == 3
        taker["s" + n] = x == 2
        plan["yr" + n] = (one(2, dz, half, PP), None, mate, one(2, dz, 1 - half, PP))
        sender["yr" + n] = taker["yr" + n] = x == 3
        plan["yq" + n] = (one(-1, dz, half, RR), None, mate, one(-1, dz, 1 - half, RR))
        sender["yq" + n] = taker["yq" + n] = x >= 1
    for j in (0, 1, 2, 3):
        d = 1 if j in UPWARD else -1
        part = (lambda dz: one(-1, dz, half, RR)) if j == 1 else (lambda dz, j=j: pair(-j, dz, RR))
        plan["RR" + str(j)] = (part(-d), None, along[d], part(2))
        if j:
            sender["RR" + str(j)] = taker["RR" + str(j)] = x >= j

    def copy(name, landing):
        source, target, device, lands = plan[name]
        n = INDEX[name]
        return pltpu.make_async_remote_copy(
            src_ref=lands if landing else source,
            dst_ref=lands if landing else (source if target is None else target),
            send_sem=send_sem.at[n],
            recv_sem=recv_sem.at[n],
            device_id=device,
            device_id_type=MESH,
        )

    def guarded(rule, name, act):
        if name in rule:
            pl.when(rule[name])(act)
        else:
            act()

    def send(*names):
        for name in names:
            guarded(sender, name, lambda name=name: copy(name, False).start())

    waited = []

    def take(*names):
        for name in names:
            guarded(taker, name, lambda name=name: copy(name, True).wait_recv())
            waited.append(name)

    def run(steps):
        for step in steps:
            (take if step[0] == "-" else send)(step[1:])

    first = [step[0] for step in BEFORE].index("-")
    run(BEFORE[:first])

    @pl.loop(0, 32)
    def _(s):
        marks[s] = seen(vert, s)

    @pl.loop(0, 8)
    def _(h):
        for k in range(8):
            name = vert[h, k]
            lower = marks[(name >> 3) & 31] & ((jnp.int32(1) << (name & 7)) - 1)
            lower = lower - ((lower >> 1) & 0x55)
            lower = (lower & 0x33) + ((lower >> 2) & 0x33)
            place[h, k] = (name >> 3) & 31
            place[8 + h, k] = 2 * ((lower + (lower >> 4)) & 3)

    run(BEFORE[first:])
    for head in heads:
        head.wait()

    near_put(0, 0, slab, slash, q, ext, stage)

    @pl.loop(0, 64 // NEAR_STEPS)
    def _(t):
        for when, steps in DURING.items():
            pl.when(t == when)(functools.partial(run, steps))
        for u in range(NEAR_STEPS):
            e = t * NEAR_STEPS + u
            near_put((u + 1) % 2, jnp.minimum(e + 1, 63), slab, slash, q, ext, stage)
            near_finish(u % 2, e, slab, slash, ext, acc, top, tot, stage)

    run(AFTER)
    take(*[name for name in NAMES if name not in waited])

    def quarter(h, n):
        return out.at[h, pl.ds(((group + n) % 4) * 256, 256)]

    def column(h):
        return out_hbm.at[:, pl.ds(pl.multiple_of((group * 8 + h) * BLK, BLK), BLK)]

    def share(h, n):
        return pltpu.make_async_remote_copy(
            src_ref=quarter(h, n),
            dst_ref=column(h),
            send_sem=part_sem.at[h, n - 1],
            recv_sem=part_recv.at[h, n - 1],
            device_id=peers[n - 1],
            device_id_type=MESH,
        )

    def keep(h):
        return pltpu.make_async_copy(quarter(h, 0), column(h), keep_sem.at[h])

    far_put(0, 0, slab, slash, vert, place, q, far, stage, spots)

    @pl.loop(0, 8)
    def _(h):
        @pl.loop(0, 8 // FAR_STEPS)
        def _(t):
            for u in range(FAR_STEPS):
                e = h * 8 + t * FAR_STEPS + u
                far_put((u + 1) % 2, jnp.minimum(e + 1, 63), slab, slash, vert, place, q, far, stage, spots)
                far_finish(u % 2, e, far, acc, top, tot, out, stage, spots)
            for n in (2, 1, 3):
                pl.when(((group + n) % 4) // 2 == t)(lambda n=n: share(h, n).start())
            pl.when(group // 2 == t)(lambda: keep(h).start())


    for name in NAMES:
        guarded(sender, name, lambda name=name: copy(name, False).wait_send())

    @pl.loop(0, 8)
    def _(h):
        keep(h).wait()
        for n in (1, 2, 3):
            origin = (group - n + 4) % 4
            share(h, n).wait_send()
            lands = out_hbm.at[:, pl.ds(pl.multiple_of((origin * 8 + h) * BLK, BLK), BLK)]
            pltpu.make_async_remote_copy(
                src_ref=quarter(h, n),
                dst_ref=lands,
                send_sem=part_sem.at[h, n - 1],
                recv_sem=part_recv.at[h, n - 1],
                device_id=peers[n - 1],
                device_id_type=MESH,
            ).wait_recv()


def attention(slash, vert, q, k, v):
    whole = pl.BlockSpec(memory_space=pl.ANY)
    scalars = pl.BlockSpec(memory_space=pltpu.SMEM)
    return pl.pallas_call(
        kernel,
        out_shape=jax.ShapeDtypeStruct((256, 4096), BF16),
        in_specs=[scalars] * 2 + [whole] * 3,
        out_specs=whole,
        scratch_shapes=[
            pltpu.VMEM((8, 1024, 128), BF16),
            pltpu.VMEM((8, 128, 128), BF16),
            pltpu.VMEM((8, 2, 128, 128), BF16),
            pltpu.VMEM((36, 2, 128, 128), BF16),
            pltpu.VMEM((32, 8, 128, 128), BF16),
            pltpu.VMEM((8, 1024, 128), F32),
            pltpu.VMEM((8, 1024, 1), F32),
            pltpu.VMEM((8, 1024, 1), F32),
            pltpu.VMEM((8, 1024, 128), BF16),
            pltpu.VMEM((2, 9, 128, 128), F32),
            pltpu.SMEM((2, 16), jnp.int32),
            pltpu.SMEM((32,), jnp.int32),
            pltpu.SMEM((16, 8), jnp.int32),
            pltpu.SemaphoreType.DMA((11,)),
            pltpu.SemaphoreType.DMA((len(NAMES),)),
            pltpu.SemaphoreType.DMA((len(NAMES),)),
            pltpu.SemaphoreType.DMA((8, 3)),
            pltpu.SemaphoreType.DMA((8, 3)),
            pltpu.SemaphoreType.DMA((8,)),
        ],
        compiler_params=pltpu.CompilerParams(
            collective_id=0, has_side_effects=True, vmem_limit_bytes=60 * 2**20
        ),
    )(slash, vert, q, k, v)


def shards(queries, keys, values, vertical, slash):
    return attention(
        slash, vertical, queries, keys.reshape(8, BLK, BLK), values.reshape(8, BLK, BLK)
    )


def solution(mesh):
    return jax.shard_map(
        shards,
        mesh=mesh,
        in_specs=(P("seq", "head"), P("seq", "head"), P("seq", "head"), P("head", None), P("head", None)),
        out_specs=P(("seq", "head"), None),
        check_vma=False,
    )
```

```python
import functools, math
import jax, jax.numpy as jnp
from jax import lax
from jax.experimental import pallas as pl
from jax.experimental.pallas import tpu as pltpu
from jax.sharding import PartitionSpec as P

BLK = 128
NEG = -1e30
BACK = 28
F32 = jnp.float32
BF16 = jnp.bfloat16
SCALE2 = math.log2(math.e) / math.sqrt(128.0)


def dot(a, b):
    return jnp.dot(a, b, preferred_element_type=F32)


def lane_max(parts):
    top = parts[0]
    for part in parts[1:]:
        top = jnp.maximum(top, part)
    return jnp.max(top, axis=1, keepdims=True)


def lane_sum(parts):
    total = parts[0]
    for part in parts[1:]:
        total = total + part
    return jnp.sum(total, axis=1, keepdims=True)


def cat_dot(ps, vs):
    return dot(jnp.concatenate([p.astype(BF16) for p in ps], axis=1), jnp.concatenate(vs, axis=0))

def near_scores(h, i, slab, slash_ref, q_ref, ext_ref):
    rows = pl.ds(pl.multiple_of(i * BLK, BLK), BLK)
    q = q_ref[h, rows, :]
    row = lax.broadcasted_iota(jnp.int32, (BLK, BLK), 0)
    col = lax.broadcasted_iota(jnp.int32, (BLK, BLK), 1)
    own = BACK + i
    blocks = [own]
    bias = []
    for k in range(8):
        off = slash_ref[h, k]
        ok = slab * 8 + i - off >= 0
        blocks.append(jnp.where(ok, own - off, own))
        bias.append(jnp.where(ok, 0.0, NEG).astype(F32))
    scores = [jnp.where(row >= col, dot(q, ext_ref[own, 0]), NEG)]
    for k in range(0, 8, 2):
        both = dot(q, jnp.concatenate([ext_ref[blocks[1 + k], 0], ext_ref[blocks[2 + k], 0]], axis=1))
        scores.append(both[:, :BLK] + bias[k])
        scores.append(both[:, BLK:] + bias[k + 1])
    return scores, blocks, rows

def far_scores(h, i, slab, slash_ref, vert_ref, pos_ref, q_ref, far_ref):
    rows = pl.ds(pl.multiple_of(i * BLK, BLK), BLK)
    q = q_ref[h, rows, :]
    mine = slab * 8 + i
    bias, places = [], []
    for k in range(8):
        gap = mine - vert_ref[h, k]
        ok = gap > 0
        for n in range(8):
            ok = ok & (slash_ref[h, n] != gap)
        bias.append(jnp.where(ok, 0.0, NEG).astype(F32))
        places.append((jnp.where(ok, pos_ref[h, k], slab), jnp.where(ok, pos_ref[8 + h, k], 0)))
    scores = []
    for k in range(0, 8, 2):
        both = dot(q, jnp.concatenate([far_ref[places[k][0], places[k][1]], far_ref[places[k + 1][0], places[k + 1][1]]], axis=1))
        scores.append(both[:, :BLK] + bias[k])
        scores.append(both[:, BLK:] + bias[k + 1])
    return scores, places, rows

def near_put(slot, e, slab, slash, q, ext, stage):
    scores, _, _ = near_scores(e // 8, e % 8, slab, slash, q, ext)
    for k, s in enumerate(scores):
        stage[slot, k] = s


def near_finish(slot, e, slab, slash, ext, acc, top, tot, stage):
    h, i = e // 8, e % 8
    rows = pl.ds(pl.multiple_of(i * BLK, BLK), BLK)
    own = BACK + i
    blocks = [own]
    for k in range(8):
        off = slash[h, k]
        blocks.append(jnp.where(slab * 8 + i - off >= 0, own - off, own))
    scores = [stage[slot, k] for k in range(9)]
    best = lane_max(scores)
    weights = [jnp.exp2((s - best) * SCALE2) for s in scores]
    acc[h, rows, :] = cat_dot(weights, [ext[b, 1] for b in blocks])
    top[h, rows, :] = best
    tot[h, rows, :] = lane_sum(weights)


def far_put(slot, e, slab, slash, vert, pos, q, far, stage, spots):
    scores, places, _ = far_scores(e // 8, e % 8, slab, slash, vert, pos, q, far)
    for k, s in enumerate(scores):
        stage[slot, k] = s
        spots[slot, k] = places[k][0]
        spots[slot, 8 + k] = places[k][1]


def far_finish(slot, e, far, acc, top, tot, out, stage, spots):
    h, i = e // 8, e % 8
    rows = pl.ds(pl.multiple_of(i * BLK, BLK), BLK)
    scores = [stage[slot, k] for k in range(8)]
    old = top[h, rows, :]
    best = jnp.maximum(old, lane_max(scores))
    keep = jnp.exp2((old - best) * SCALE2)
    weights = [jnp.exp2((s - best) * SCALE2) for s in scores]
    mixed = cat_dot(weights, [far[spots[slot, k], spots[slot, 8 + k] + 1] for k in range(8)])
    total = tot[h, rows, :] * keep + lane_sum(weights)
    out[h, rows, :] = ((acc[h, rows, :] * keep + mixed) / total).astype(BF16)


MESH = pl.DeviceIdType.MESH
NEAR_STEPS = 4
FAR_STEPS = 4
DIRS = (1, -1)
NAMES = ["y", "zP2", "hA", "hB", "h3", "h4", "y1", "y2", "y3", "ro", "rp"]
NAMES += [kind + str(d) for kind in ("xo", "xp", "x1", "x2", "x3") for d in DIRS]
NAMES += [kind + n for kind in ("r", "s", "yr", "yq") for n in "123"]
NAMES += ["R" + str(j) + str(d) for j in (1, 2, 3) for d in DIRS]
NAMES += ["RR" + str(j) for j in (0, 1, 2, 3)]
NAMES += [kind + str(d) + n for kind in ("zP", "R0") for d in DIRS for n in "op"]
UPWARD = (2,)
BEFORE = (
    "+y", "+hA", "+hB", "+xo-1", "+zP-1o", "+R0-1o", "+xo1", "-y",
    "+xp-1", "+zP-1p", "+zP1o", "+zP1p", "-hA", "+y1", "+R0-1p", "-xo-1",
    "+ro", "-hB", "+h4", "-xp-1", "+rp", "-zP-1o", "-zP-1p", "+zP2",
    "-y1", "+h3", "+y2", "+x1-1", "-xo1", "+R11", "+x11", "+R3-1",
    "-zP2", "+x2-1", "+x21", "+R01p", "-h4", "+y3", "-zP1o", "-zP1p",
    "+x3-1", "-ro", "-rp", "+R21", "+R1-1", "-R1-1", "+RR1", "+yq1",
    "+x31", "-R0-1o", "-R0-1p", "+RR0", "-x1-1", "+r1", "-h3", "-y2",
    "-y3",
)
DURING = {
    1: ("-x2-1", "+r2",),
    2: ("+R01o",),
    3: ("+s2", "-RR1", "+yq2", "+xp1", "-R11", "+yq3",),
    6: ("+R31", "-R3-1", "+RR3",),
    7: ("+R2-1", "-x3-1", "+r3",),
    8: ("-R21", "+RR2", "+s1",),
    9: ("-r1", "+yr1",),
    11: ("-r2", "+yr2", "+s3",),
    12: ("-r3", "+yr3",),
}
AFTER = (
    "-R01o", "-R01p", "-xp1", "-x11", "-x21", "-x31", "-R31", "-R2-1",
    "-s1", "-yr1", "-yq1", "-s2", "-yr2", "-yq2", "-s3", "-yr3",
    "-yq3", "-RR0", "-RR2", "-RR3",
)
INDEX = {name: n for n, name in enumerate(NAMES)}


def seen(vert, slab):
    mask = jnp.int32(0)
    for h in range(8):
        for k in range(8):
            name = vert[h, k]
            mask = mask | jnp.where((name >> 3) == slab, jnp.int32(1) << (name & 7), 0)
    return mask


def kernel(slash, vert, q_hbm, k_hbm, v_hbm, out_hbm,
           q, raw, own, ext, far, acc, top, tot, out, stage, spots, marks, place, load_sem, send_sem, recv_sem, part_sem, part_recv, keep_sem):
    group = lax.axis_index("head")
    slab = lax.axis_index("seq")
    x, z, half = slab // 8, (slab // 2) % 4, slab % 2
    loads = [
        pltpu.make_async_copy(k_hbm, raw, load_sem.at[8]),
        pltpu.make_async_copy(v_hbm, own.at[:, 1], load_sem.at[9]),
        pltpu.make_async_copy(v_hbm, ext.at[pl.ds(BACK, 8), 1], load_sem.at[10]),
    ]
    heads = [
        pltpu.make_async_copy(q_hbm.at[:, pl.ds(h * BLK, BLK)], q.at[h], load_sem.at[h]) for h in range(8)
    ]
    for load in loads + heads:
        load.start()

    def seat(dx, dz, dy):
        return ((x + dx) % 4) * 8 + ((z + dz) % 4) * 2 + ((half + dy) % 2)

    def spot(g, s):
        return (g, s)

    mate = spot(group, seat(0, 0, 1))
    after = spot(group, (slab + 2) % 32)
    before = spot(group, (slab + 30) % 32)
    across = {d: spot(group, seat(d, 0, 0)) for d in DIRS}
    along = {d: spot(group, seat(0, d, 0)) for d in DIRS}
    peers = [spot((group + n) % 4, slab) for n in (1, 2, 3)]
    barrier = pltpu.get_barrier_semaphore()
    friends = [mate, after, before, across[1], across[-1], along[1], along[-1]] + peers
    for friend in friends:
        pl.semaphore_signal(barrier, inc=1, device_id=friend, device_id_type=MESH)

    mask, count, chosen = seen(vert, slab), jnp.int32(0), [jnp.int32(0)] * 4
    for b in range(8):
        bit = (mask >> b) & 1
        for c in range(4):
            chosen[c] = jnp.where((bit == 1) & (count == c), b, chosen[c])
        count = count + bit

    for load in loads:
        load.wait()
    for b in range(8):
        flipped = raw[b].astype(F32).T.astype(BF16)
        own[b, 0] = flipped
        ext[BACK + b, 0] = flipped
    for c in range(4):
        far[slab, 2 * c] = own[chosen[c], 0]
        far[slab, 2 * c + 1] = own[chosen[c], 1]
    pl.semaphore_wait(barrier, len(friends))

    PP, RR, ALL = (0, 4), (4, 4), (0, 8)

    def one(dx, dz, side, sub):
        return far.at[pl.ds(((x + dx) % 4) * 8 + ((z + dz) % 4) * 2 + side, 1), pl.ds(*sub)]

    def pair(dx, dz, sub):
        return far.at[pl.ds(((x + dx) % 4) * 8 + ((z + dz) % 4) * 2, 2), pl.ds(*sub)]

    def near(at, side_step=0):
        return ext.at[pl.ds(at + side_step * half, 4)]

    plan = {
        "y": (one(0, 0, half, ALL), None, mate, one(0, 0, 1 - half, ALL)),
        "zP2": (pair(0, 1, PP), None, along[-1], pair(0, 2, PP)),
        "hA": (near(28), near(12), after, near(12)),
        "hB": (near(32), near(16), after, near(16)),
        "h4": (near(16), near(0), after, near(0)),
        "h3": (near(20), near(4), after, near(4)),
        "y1": (near(28, -16), near(20), mate, near(20)),
        "y2": (near(32, -16), near(24), mate, near(24)),
        "y3": (near(16, -16), near(8), mate, near(8)),
    }
    sends = {d: x < 3 if d == 1 else x < 2 for d in DIRS}
    takes = {d: x > 0 if d == 1 else (x == 3) | (x == 0) for d in DIRS}
    sender, taker = {}, {}
    for d in DIRS:
        for n, source, lands in (
            ("xo", one(0, 0, half, ALL), one(-d, 0, half, ALL)),
            ("xp", one(0, 0, 1 - half, ALL), one(-d, 0, 1 - half, ALL)),
            ("x1", pair(0, 1, PP), pair(-d, 1, PP)),
            ("x2", pair(0, 2, PP), pair(-d, 2, PP)),
            ("x3", pair(0, -1, PP), pair(-d, -1, PP)),
        ):
            plan[n + str(d)] = (source, None, across[d], lands)
            sender[n + str(d)] = sends[d]
            taker[n + str(d)] = takes[d]
        for n, side in (("o", half), ("p", 1 - half)):
            plan["zP" + str(d) + n] = (one(0, 0, side, PP), None, along[d], one(0, -d, side, PP))
            plan["R0" + str(d) + n] = (one(0, 0, side, RR), None, along[d], one(0, -d, side, RR))
        for j in (1, 2, 3):
            part = (lambda dz: one(-1, dz, half, RR)) if j == 1 else (lambda dz, j=j: pair(-j, dz, RR))
            plan["R" + str(j) + str(d)] = (part(0), None, along[d], part(-d))
            sender["R" + str(j) + str(d)] = taker["R" + str(j) + str(d)] = x >= j
    for n, source, lands in (
        ("ro", one(1, 0, half, ALL), one(2, 0, half, ALL)),
        ("rp", one(1, 0, 1 - half, ALL), one(2, 0, 1 - half, ALL)),
        ("r1", one(1, 1, half, PP), one(2, 1, half, PP)),
        ("r2", one(1, 2, half, PP), one(2, 2, half, PP)),
        ("r3", one(1, -1, half, PP), one(2, -1, half, PP)),
    ):
        plan[n] = (source, None, across[-1], lands)
        sender[n] = (x == 0) | (x == 3)
        taker[n] = (x == 3) | (x == 2)
    for n, dz in (("1", 1), ("2", 2), ("3", -1)):
        plan["s" + n] = (one(1, dz, 1 - half, PP), None, across[-1], one(2, dz, 1 - half, PP))
        sender["s" + n] = x == 3
        taker["s" + n] = x == 2
        plan["yr" + n] = (one(2, dz, half, PP), None, mate, one(2, dz, 1 - half, PP))
        sender["yr" + n] = taker["yr" + n] = x == 3
        plan["yq" + n] = (one(-1, dz, half, RR), None, mate, one(-1, dz, 1 - half, RR))
        sender["yq" + n] = taker["yq" + n] = x >= 1
    for j in (0, 1, 2, 3):
        d = 1 if j in UPWARD else -1
        part = (lambda dz: one(-1, dz, half, RR)) if j == 1 else (lambda dz, j=j: pair(-j, dz, RR))
        plan["RR" + str(j)] = (part(-d), None, along[d], part(2))
        if j:
            sender["RR" + str(j)] = taker["RR" + str(j)] = x >= j

    def copy(name, landing):
        source, target, device, lands = plan[name]
        n = INDEX[name]
        return pltpu.make_async_remote_copy(
            src_ref=lands if landing else source,
            dst_ref=lands if landing else (source if target is None else target),
            send_sem=send_sem.at[n],
            recv_sem=recv_sem.at[n],
            device_id=device,
            device_id_type=MESH,
        )

    def guarded(rule, name, act):
        if name in rule:
            pl.when(rule[name])(act)
        else:
            act()

    def send(*names):
        for name in names:
            guarded(sender, name, lambda name=name: copy(name, False).start())

    waited = []

    def take(*names):
        for name in names:
            guarded(taker, name, lambda name=name: copy(name, True).wait_recv())
            waited.append(name)

    def run(steps):
        for step in steps:
            (take if step[0] == "-" else send)(step[1:])

    first = [step[0] for step in BEFORE].index("-")
    run(BEFORE[:first])

    @pl.loop(0, 32)
    def _(s):
        marks[s] = seen(vert, s)

    @pl.loop(0, 8)
    def _(h):
        for k in range(8):
            name = vert[h, k]
            lower = marks[(name >> 3) & 31] & ((jnp.int32(1) << (name & 7)) - 1)
            lower = lower - ((lower >> 1) & 0x55)
            lower = (lower & 0x33) + ((lower >> 2) & 0x33)
            place[h, k] = (name >> 3) & 31
            place[8 + h, k] = 2 * ((lower + (lower >> 4)) & 3)

    run(BEFORE[first:])
    for head in heads:
        head.wait()

    near_put(0, 0, slab, slash, q, ext, stage)

    @pl.loop(0, 64 // NEAR_STEPS)
    def _(t):
        for when, steps in DURING.items():
            pl.when(t == when)(functools.partial(run, steps))
        for u in range(NEAR_STEPS):
            e = t * NEAR_STEPS + u
            near_put((u + 1) % 2, jnp.minimum(e + 1, 63), slab, slash, q, ext, stage)
            near_finish(u % 2, e, slab, slash, ext, acc, top, tot, stage)

    run(AFTER)
    take(*[name for name in NAMES if name not in waited])

    def quarter(h, n):
        return out.at[h, pl.ds(((group + n) % 4) * 256, 256)]

    def column(h):
        return out_hbm.at[:, pl.ds(pl.multiple_of((group * 8 + h) * BLK, BLK), BLK)]

    def share(h, n):
        return pltpu.make_async_remote_copy(
            src_ref=quarter(h, n),
            dst_ref=column(h),
            send_sem=part_sem.at[h, n - 1],
            recv_sem=part_recv.at[h, n - 1],
            device_id=peers[n - 1],
            device_id_type=MESH,
        )

    def keep(h):
        return pltpu.make_async_copy(quarter(h, 0), column(h), keep_sem.at[h])

    turn = 4 * (1 - group // 2)

    def turned(e):
        return (e // 8) * 8 + (e + turn) % 8

    far_put(0, turned(0), slab, slash, vert, place, q, far, stage, spots)

    @pl.loop(0, 8)
    def _(h):
        @pl.loop(0, 8 // FAR_STEPS)
        def _(t):
            for u in range(FAR_STEPS):
                e = h * 8 + t * FAR_STEPS + u
                far_put((u + 1) % 2, turned(jnp.minimum(e + 1, 63)), slab, slash, vert, place, q, far, stage, spots)
                far_finish(u % 2, turned(e), far, acc, top, tot, out, stage, spots)
            for n in (2, 1, 3):
                pl.when((((group + n) % 4) // 2 + group // 2 + 1 + t) % 2 == 0)(lambda n=n: share(h, n).start())
            pl.when(t == 1)(lambda: keep(h).start())


    for name in NAMES:
        guarded(sender, name, lambda name=name: copy(name, False).wait_send())

    @pl.loop(0, 8)
    def _(h):
        keep(h).wait()
        for n in (1, 2, 3):
            origin = (group - n + 4) % 4
            share(h, n).wait_send()
            lands = out_hbm.at[:, pl.ds(pl.multiple_of((origin * 8 + h) * BLK, BLK), BLK)]
            pltpu.make_async_remote_copy(
                src_ref=quarter(h, n),
                dst_ref=lands,
                send_sem=part_sem.at[h, n - 1],
                recv_sem=part_recv.at[h, n - 1],
                device_id=peers[n - 1],
                device_id_type=MESH,
            ).wait_recv()


def attention(slash, vert, q, k, v):
    whole = pl.BlockSpec(memory_space=pl.ANY)
    scalars = pl.BlockSpec(memory_space=pltpu.SMEM)
    return pl.pallas_call(
        kernel,
        out_shape=jax.ShapeDtypeStruct((256, 4096), BF16),
        in_specs=[scalars] * 2 + [whole] * 3,
        out_specs=whole,
        scratch_shapes=[
            pltpu.VMEM((8, 1024, 128), BF16),
            pltpu.VMEM((8, 128, 128), BF16),
            pltpu.VMEM((8, 2, 128, 128), BF16),
            pltpu.VMEM((36, 2, 128, 128), BF16),
            pltpu.VMEM((32, 8, 128, 128), BF16),
            pltpu.VMEM((8, 1024, 128), F32),
            pltpu.VMEM((8, 1024, 1), F32),
            pltpu.VMEM((8, 1024, 1), F32),
            pltpu.VMEM((8, 1024, 128), BF16),
            pltpu.VMEM((2, 9, 128, 128), F32),
            pltpu.SMEM((2, 16), jnp.int32),
            pltpu.SMEM((32,), jnp.int32),
            pltpu.SMEM((16, 8), jnp.int32),
            pltpu.SemaphoreType.DMA((11,)),
            pltpu.SemaphoreType.DMA((len(NAMES),)),
            pltpu.SemaphoreType.DMA((len(NAMES),)),
            pltpu.SemaphoreType.DMA((8, 3)),
            pltpu.SemaphoreType.DMA((8, 3)),
            pltpu.SemaphoreType.DMA((8,)),
        ],
        compiler_params=pltpu.CompilerParams(
            collective_id=0, has_side_effects=True, vmem_limit_bytes=60 * 2**20
        ),
    )(slash, vert, q, k, v)


def shards(queries, keys, values, vertical, slash):
    return attention(
        slash, vertical, queries, keys.reshape(8, BLK, BLK), values.reshape(8, BLK, BLK)
    )


def solution(mesh):
    return jax.shard_map(
        shards,
        mesh=mesh,
        in_specs=(P("seq", "head"), P("seq", "head"), P("seq", "head"), P("head", None), P("head", None)),
        out_specs=P(("seq", "head"), None),
        check_vma=False,
    )
```
